32 devices in a mesh: seg: 16 (over z, x, core), freq: 2 (over y).
Axes of the slice: x: 2, y: 2, z: 4, core: 2. Of those that a mesh axis runs over, the one named last changes fastest.
Arguments:
- coarse: float32 [64, 128, 2048], P('seg', None, 'freq'), may hold values from 0.5 to 8
- offsets: int32 [64, 32], replicated, may hold values from -8 to 8, as said below
Outputs:
- fine: float32 [32, 128, 2048], P(None, 'seg', 'freq')
- peaks: float32 [128], P('seg')
The draws below stay inside these ranges and needn't reach their ends.
Inputs may be any that keep to these rules, and one draw needn't show every extreme that they name: `offsets`: every entry lies in -8 to 8, and both ends occur in every draw.
All inputs are finite; a program needn't handle non-finite values.
Results may differ from the reference program's by a relative error of at most 0.0003.
Values sent between devices are 32-bit elements; how exact they have to be, the bound alone decides.
A program may use at most 128 MiB of HBM per device.

```python
import math
import jax
import jax.numpy as jnp
from jax import lax

SPINDOWNS = 32
HALO = 8
SEGMENTS = 64
SKY_POINTS = 128
BINS = 2048


def draw_offsets(key, part):
    base = jax.random.randint(jax.random.fold_in(key, 11), (SEGMENTS, SPINDOWNS), -HALO, HALO + 1, dtype=jnp.int32)
    first_seg = jax.random.randint(jax.random.fold_in(key, 12), (), 0, SEGMENTS, dtype=jnp.int32)
    step_seg = jax.random.randint(jax.random.fold_in(key, 13), (), 1, SEGMENTS, dtype=jnp.int32)
    second_seg = (first_seg + step_seg) % SEGMENTS
    first_spin = jax.random.randint(jax.random.fold_in(key, 14), (), 0, SPINDOWNS, dtype=jnp.int32)
    second_spin = jax.random.randint(jax.random.fold_in(key, 15), (), 0, SPINDOWNS, dtype=jnp.int32)
    base = base.at[first_seg, first_spin].set(HALO)
    base = base.at[second_seg, second_spin].set(-HALO)
    return base


def shard_levels(stream_key, shape, pieces, smallest, largest):
    gain = 1.0
    for dim, parts in pieces:
        steps = jax.random.uniform(jax.random.fold_in(jax.random.fold_in(stream_key, 6), dim), (parts,), jnp.float32, smallest / len(pieces), largest / len(pieces))
        gain = gain * jnp.repeat(jnp.exp(steps), shape[dim] // parts).reshape((-1,) + (1,) * (len(shape) - 1 - dim))
    return gain


def setup_inputs(seed: int = 0) -> dict:
    streams_of = jax.random.split(jax.random.key(seed), 3)
    coarse = jnp.clip(jnp.exp(math.log(8.0) - 2.7725887 * jax.random.uniform(streams_of[0], (SEGMENTS, SKY_POINTS, BINS), jnp.float32) ** shard_levels(streams_of[0], (SEGMENTS, SKY_POINTS, BINS), ((0, 16), (2, 2)), -0.2, 0.2)), 0.5, 8.0)
    offsets = draw_offsets(jax.random.fold_in(streams_of[2], 71), 0)
    return {"coarse": coarse, "offsets": offsets}


def window(line, begin):
    return lax.dynamic_slice_in_dim(line, begin, line.shape[1] - 2 * HALO, 1)


def reference(coarse, offsets):
    padded = jnp.pad(coarse, ((0, 0), (0, 0), (HALO, HALO)))

    def spindown(column):
        starts = (HALO + column).astype(jnp.int32)
        shifted = jax.vmap(window)(padded, starts)
        return jnp.sum(shifted, axis=0) / SEGMENTS

    fine = lax.map(spindown, offsets.T)
    peaks = jnp.max(fine, axis=(0, 2))
    return fine, peaks
```

```python
import functools

import jax
import jax.numpy as jnp
from jax import lax
from jax.experimental import pallas as pl
from jax.experimental.pallas import tpu as pltpu
from jax.sharding import PartitionSpec as P

HALO = 8
EDGE = 128
SHIFTS = 2 * HALO + 1
PLANES = 4
LEAD = 2
MESH = pl.DeviceIdType.MESH


def partner(me, step, count):
    result = me
    bit = 1
    while bit < count:
        wanted = (step // bit) % 2 if isinstance(step, int) else lax.rem(step // bit, 2)
        held = lax.rem(me // bit, 2)
        result = result + bit * wanted * (1 - 2 * held)
        bit *= 2
    return result


def kernel(
    nseg,
    nfreq,
    tail,
    coarse,
    offsets,
    total,
    tops,
    maps,
    low,
    high,
    shifted,
    shifts,
    own_sem,
    shifts_sem,
    send_sem,
    edge_recv,
    bulk_recv,
    tail_recv,
    up_send,
    up_recv,
    down_send,
    down_recv,
    top_send,
    top_recv,
    near_sem,
    far_sem,
):
    local_segs = coarse.shape[0]
    spins, rows, bins = total.shape
    scale = 1.0 / (nseg * local_segs)
    size = nseg // PLANES
    bulk = local_segs - tail
    me = lax.axis_index("seg")
    band = lax.axis_index("freq")
    plane = me // size
    inner = lax.rem((plane + 1) // 2, 2) == 1
    outer = jnp.logical_not(inner)

    early = EDGE if nfreq <= 2 else bins
    edge_at = jnp.where(band == 0, bins - early, 0)
    rest_at = jnp.where(band == 0, 0, early)

    def each(group, begin, end, act):
        @pl.loop(begin, end)
        def _(j):
            act(group * size + j)

    def greet(step, sem):
        pl.semaphore_signal(
            sem, inc=1, device_id={"seg": partner(me, step, nseg), "freq": band}, device_id_type=MESH
        )

    def greet_bands(sem):
        for step in range(1, nfreq):
            pl.semaphore_signal(
                sem, inc=1, device_id={"seg": me, "freq": lax.rem(band + step, nfreq)}, device_id_type=MESH
            )

    def piece(step, begin, width, segs, received):
        other = partner(me, step, nseg)
        columns = pl.ds(pl.multiple_of(begin, EDGE), width)
        rows_of = pl.ds(pl.multiple_of(other * rows, rows), rows)
        return pltpu.make_async_remote_copy(
            src_ref=coarse.at[segs, rows_of, columns],
            dst_ref=maps.at[step, segs, :, columns],
            send_sem=send_sem,
            recv_sem=received,
            device_id={"seg": other, "freq": band},
            device_id_type=MESH,
        )

    def send_edge(step):
        piece(step, edge_at, early, pl.ds(0, local_segs), edge_recv.at[step // size]).start()

    def bulk_of(step):
        return piece(step, rest_at, bins - early, pl.ds(0, bulk), bulk_recv.at[step])

    def tail_of(step):
        return piece(step, rest_at, bins - early, pl.ds(bulk, tail), tail_recv.at[step])

    def send_bulk(step):
        if early < bins:
            bulk_of(step).start()

    def send_tail(step):
        if early < bins:
            tail_of(step).start()

    def wait_edges(group, first):
        there = maps.at[pl.ds(group * size + first, size - first), :, :, pl.ds(0, early)]
        pltpu.make_async_copy(there, there, edge_recv.at[group]).wait()

    def upward(group):
        members = pl.ds(group * size, size)
        return pltpu.make_async_remote_copy(
            src_ref=maps.at[members, :, :, pl.ds(bins - EDGE, EDGE)],
            dst_ref=low.at[members],
            send_sem=up_send,
            recv_sem=up_recv.at[group],
            device_id={"seg": me, "freq": band + 1},
            device_id_type=MESH,
        )

    def downward(group):
        members = pl.ds(group * size, size)
        return pltpu.make_async_remote_copy(
            src_ref=maps.at[members, :, :, pl.ds(0, EDGE)],
            dst_ref=high.at[members],
            send_sem=down_send,
            recv_sem=down_recv.at[group],
            device_id={"seg": me, "freq": band - 1},
            device_id_type=MESH,
        )

    def forward(group):
        @pl.when(band < nfreq - 1)
        def _():
            upward(group).start()

        @pl.when(band > 0)
        def _():
            downward(group).start()

    def wait_halo(group):
        @pl.when(band < nfreq - 1)
        def _():
            downward(group).wait_recv()

        @pl.when(band > 0)
        def _():
            upward(group).wait_recv()

    barrier = pltpu.get_barrier_semaphore()

    @pl.when(inner)
    def _():
        each(3, 0, size, lambda step: greet(step, barrier))
        each(1, 0, size, lambda step: greet(step, barrier))
        pl.semaphore_wait(barrier, size)

    @pl.when(outer)
    def _():
        greet_bands(barrier)
        pl.semaphore_wait(barrier, size + nfreq - 1)
        greet_bands(near_sem)

    first_group = jnp.where(inner, 3, 1)
    lead = min(LEAD, size)
    each(first_group, 0, size, send_edge)
    each(first_group, 0, lead, send_bulk)

    own = pltpu.make_async_copy(
        coarse.at[:, pl.ds(pl.multiple_of(me * rows, rows), rows), :], maps.at[0], own_sem
    )
    own.start()
    load_shifts = pltpu.make_async_copy(offsets, shifts, shifts_sem)
    load_shifts.start()

    @pl.when(outer)
    def _():
        if nfreq > 1:
            pl.semaphore_wait(near_sem, nfreq - 1)
        each(1, 0, size, lambda step: greet(step, near_sem))
        pl.semaphore_wait(near_sem, 1)

    @pl.when(inner)
    def _():
        pl.semaphore_wait(near_sem, size)
        greet(3 * size, far_sem)
        pl.semaphore_wait(far_sem, 1)
        greet(size, near_sem)

    each(2, 0, size, send_edge)
    each(4 - first_group, 0, size, send_edge)
    each(0, 1, size, send_edge)

    @pl.when(inner)
    def _():
        each(1, 0, size, send_bulk)
        each(1, 0, size, send_tail)
        each(0, 1, size, send_bulk)
        each(0, 1, size, send_tail)
        each(3, lead, size, send_bulk)
        each(2, 0, size, send_bulk)
        each(2, 0, size, send_tail)
        each(3, 0, size, send_tail)

    @pl.when(outer)
    def _():
        each(1, lead, size, send_bulk)
        each(1, 0, size, send_tail)
        each(0, 1, size, send_bulk)
        each(0, 1, size, send_tail)
        each(2, 0, size, send_bulk)
        each(3, 0, size, send_bulk)
        each(3, 0, size, send_tail)
        each(2, 0, size, send_tail)

    total[...] = jnp.zeros_like(total)

    @pl.when(band == 0)
    def _():
        low[...] = jnp.zeros_like(low)

    @pl.when(band == nfreq - 1)
    def _():
        high[...] = jnp.zeros_like(high)

    def add(step, begin, count, best=None):
        first = partner(me, step, nseg) * local_segs
        segs = range(begin, begin + count)
        lane = lax.broadcasted_iota(jnp.int32, (rows, EDGE), 1)
        for seg in segs:
            ring = jnp.where(lane < EDGE // 2, high[step, seg], low[step, seg])
            line = jnp.concatenate([maps[step, seg], ring], axis=1)
            width = bins + EDGE
            for shift in range(-HALO, HALO + 1):
                turned = line if shift == 0 else pltpu.roll(line, (-shift) % width, 1)
                shifted[seg, HALO + shift] = turned[:, :bins]

        def spindown(spin, best):
            value = total[spin]
            for seg in segs:
                value = value + shifted[seg, HALO + shifts[spin, first + seg]]
            if best is not None:
                value = value * scale
                best = jnp.maximum(best, value)
            total[spin] = value
            return best

        return lax.fori_loop(0, spins, spindown, best, unroll=4)

    wait_edges(first_group, 0)
    forward(first_group)
    own.wait()
    wait_edges(0, 1)
    forward(0)
    wait_edges(4 - first_group, 0)
    forward(4 - first_group)
    wait_edges(2, 0)
    forward(2)
    load_shifts.wait()

    @pl.loop(0, nseg)
    def _(turn):
        place = turn // size
        group = jnp.where(jnp.logical_and(inner, place >= 2), 5 - place, place)
        member = lax.rem(turn, size)
        step = group * size + member

        @pl.when(member == 0)
        def _():
            wait_halo(group)

        @pl.when(step > 0)
        def _():
            if early < bins:
                bulk_of(step).wait_recv()

        add(step, 0, bulk)

    def last_part(turn, best=None):
        across = turn - 2 * size
        far = (2 + lax.rem(across, 2)) * size + across // 2
        step = jnp.where(turn < 2 * size, turn, far)

        @pl.when(step > 0)
        def _():
            if early < bins:
                tail_of(step).wait_recv()

        return add(step, bulk, tail, best)

    @pl.loop(0, nseg - 1)
    def _(turn):
        last_part(turn)

    best = last_part(
        jnp.int32(nseg - 1), jnp.full((rows, bins), -jnp.inf, jnp.float32)
    )
    top = best[:, :EDGE]
    for begin in range(EDGE, bins, EDGE):
        top = jnp.maximum(top, best[:, begin : begin + EDGE])
    tops[0] = top

    def tell(step):
        return pltpu.make_async_remote_copy(
            src_ref=tops.at[0],
            dst_ref=tops.at[step],
            send_sem=top_send.at[step],
            recv_sem=top_recv.at[step],
            device_id={"seg": me, "freq": lax.rem(band + step, nfreq)},
            device_id_type=MESH,
        )

    for step in range(1, nfreq):
        tell(step).start()

    sent = coarse.at[:, pl.ds(0, (nseg - 1) * rows), :]
    pltpu.make_async_copy(sent, sent, send_sem).wait()

    @pl.when(band < nfreq - 1)
    def _():
        pltpu.make_async_copy(low, low, up_send).wait()

    @pl.when(band > 0)
    def _():
        pltpu.make_async_copy(high, high, down_send).wait()

    for step in range(1, nfreq):
        tell(step).wait()


def finish(total, tops, fine, peaks, line, sem, line_sem):
    write = pltpu.make_async_copy(total, fine, sem)
    write.start()
    bands, rows, width = tops.shape
    row = lax.broadcasted_iota(jnp.int32, (rows, width), 0)
    lane = lax.broadcasted_iota(jnp.int32, (rows, width), 1)
    top = tops[0]
    for band in range(1, bands):
        top = jnp.maximum(top, tops[band])
    top = jnp.max(top, axis=1, keepdims=True)
    line[...] = jnp.sum(jnp.where(row == lane, top, 0.0), axis=0)[:rows]
    write_line = pltpu.make_async_copy(line, peaks, line_sem)
    write_line.start()
    write.wait()
    write_line.wait()


def solution(mesh):
    nseg, nfreq = mesh.shape["seg"], mesh.shape["freq"]

    def on_device(coarse, offsets):
        local_segs, points, bins = coarse.shape
        rows = points // nseg
        spins = offsets.shape[1]
        tail = 1
        hbm = pl.BlockSpec(memory_space=pltpu.HBM)
        vmem = pl.BlockSpec(memory_space=pltpu.VMEM)
        dma = pltpu.SemaphoreType.DMA
        total, tops = pl.pallas_call(
            functools.partial(kernel, nseg, nfreq, tail),
            out_shape=(
                jax.ShapeDtypeStruct((spins, rows, bins), jnp.float32),
                jax.ShapeDtypeStruct((nfreq, rows, EDGE), jnp.float32),
            ),
            in_specs=[hbm, hbm],
            out_specs=(vmem, vmem),
            scratch_shapes=[
                pltpu.VMEM((nseg, local_segs, rows, bins), jnp.float32),
                pltpu.VMEM((nseg, local_segs, rows, EDGE), jnp.float32),
                pltpu.VMEM((nseg, local_segs, rows, EDGE), jnp.float32),
                pltpu.VMEM((local_segs, SHIFTS, rows, bins), jnp.float32),
                pltpu.SMEM(offsets.shape[::-1], jnp.int32),
                dma,
                dma,
                dma,
                dma((PLANES,)),
                dma((nseg,)),
                dma((nseg,)),
                dma,
                dma((PLANES,)),
                dma,
                dma((PLANES,)),
                dma((nfreq,)),
                dma((nfreq,)),
                pltpu.SemaphoreType.REGULAR,
                pltpu.SemaphoreType.REGULAR,
            ],
            compiler_params=pltpu.CompilerParams(
                collective_id=0, has_side_effects=True, vmem_limit_bytes=32 << 20
            ),
        )(pltpu.with_memory_space_constraint(coarse, pltpu.HBM), pltpu.with_memory_space_constraint(offsets.T, pltpu.HBM))
        return pl.pallas_call(
            finish,
            out_shape=(
                jax.ShapeDtypeStruct((spins, rows, bins), jnp.float32),
                jax.ShapeDtypeStruct((rows,), jnp.float32),
            ),
            in_specs=[vmem, vmem],
            out_specs=(hbm, hbm),
            scratch_shapes=[pltpu.VMEM((rows,), jnp.float32), dma, dma],
            compiler_params=pltpu.CompilerParams(vmem_limit_bytes=8 << 20),
        )(total, tops)

    return jax.shard_map(
        on_device,
        mesh=mesh,
        in_specs=(P("seg", None, "freq"), P()),
        out_specs=(P(None, "seg", "freq"), P("seg")),
        check_vma=False,
    )
```

```python
import functools

import jax
import jax.numpy as jnp
from jax import lax
from jax.experimental import pallas as pl
from jax.experimental.pallas import tpu as pltpu
from jax.sharding import PartitionSpec as P

HALO = 8
EDGE = 128
SHIFTS = 2 * HALO + 1
PLANES = 4
PAIR = 2
MESH = pl.DeviceIdType.MESH


def partner(me, step, count):
    result = me
    bit = 1
    while bit < count:
        wanted = (step // bit) % 2 if isinstance(step, int) else lax.rem(step // bit, 2)
        held = lax.rem(me // bit, 2)
        result = result + bit * wanted * (1 - 2 * held)
        bit *= 2
    return result


def kernel(
    nseg,
    nfreq,
    parts,
    coarse,
    offsets,
    total,
    maps,
    low,
    high,
    shifted,
    tops,
    shifts,
    own_sem,
    shifts_sem,
    send_sem,
    edge_recv,
    pair_recv,
    part_recv,
    halo_send,
    halo_recv,
    top_send,
    top_recv,
    near_sem,
    far_sem,
    band_sem,
):
    local_segs = coarse.shape[0]
    spins = total.shape[0] - 1
    rows, bins = total.shape[1:]
    scale = 1.0 / (nseg * local_segs)
    size = nseg // PLANES
    begins = [sum(parts[:place]) for place in range(len(parts))]
    me = lax.axis_index("seg")
    band = lax.axis_index("freq")
    plane = me // size
    inner = lax.rem((plane + 1) // 2, 2) == 1
    outer = jnp.logical_not(inner)
    last_group = jnp.where(inner, 3, 2)
    last = (last_group + 1) * size - PAIR

    early = EDGE if nfreq <= 2 else bins
    width = bins - early
    edge_at = jnp.where(band == 0, bins - early, 0)
    rest_at = jnp.where(band == 0, 0, early)

    def each(begin, end, act):
        @pl.loop(begin, end)
        def _(step):
            act(step)

    def greet(step, sem):
        pl.semaphore_signal(
            sem, inc=1, device_id={"seg": partner(me, step, nseg), "freq": band}, device_id_type=MESH
        )

    def greet_bands(sem):
        for step in range(1, nfreq):
            pl.semaphore_signal(
                sem, inc=1, device_id={"seg": me, "freq": lax.rem(band + step, nfreq)}, device_id_type=MESH
            )

    def send(step, begin, count, first, segs, received):
        other = partner(me, step, nseg)
        columns = pl.ds(pl.multiple_of(begin, EDGE), count)
        rows_of = pl.ds(pl.multiple_of(other * rows, rows), rows)
        members = pl.ds(first, segs)
        pltpu.make_async_remote_copy(
            src_ref=coarse.at[members, rows_of, columns],
            dst_ref=maps.at[step, members, :, columns],
            send_sem=send_sem,
            recv_sem=received,
            device_id={"seg": other, "freq": band},
            device_id_type=MESH,
        ).start()

    def send_edge(step):
        send(step, edge_at, early, 0, local_segs, edge_recv.at[step // size])

    def send_rest(step):
        if width:
            send(step, rest_at, width, 0, local_segs, pair_recv.at[step // PAIR])

    def part_sem(pair, place):
        return part_recv.at[place - 1] if place else pair_recv.at[pair]

    def send_parts(group):
        core = lax.rem(me, PAIR)
        first = (group + 1) * size - PAIR
        if width:
            for place, segs in enumerate(parts):
                for turn in range(PAIR):
                    step = first + lax.rem(core + turn, PAIR)
                    send(step, rest_at, width, begins[place], segs, part_sem(first // PAIR, place))

    def wait_for(there, sem):
        pltpu.make_async_copy(there, there, sem).wait()

    def wait_edges(group, first):
        wait_for(maps.at[pl.ds(group * size + first, size - first), :, :, pl.ds(0, early)], edge_recv.at[group])

    def wait_rest(step, steps, segs, sem):
        if width:
            wait_for(maps.at[pl.ds(step, steps), pl.ds(0, segs), :, pl.ds(0, width)], sem)

    def upward(group):
        members = pl.ds(group * size, size)
        return pltpu.make_async_remote_copy(
            src_ref=maps.at[members, :, :, pl.ds(bins - EDGE, EDGE)],
            dst_ref=low.at[members],
            send_sem=halo_send.at[0],
            recv_sem=halo_recv.at[0, group],
            device_id={"seg": me, "freq": band + 1},
            device_id_type=MESH,
        )

    def downward(group):
        members = pl.ds(group * size, size)
        way = halo_send.shape[0] - 1
        return pltpu.make_async_remote_copy(
            src_ref=maps.at[members, :, :, pl.ds(0, EDGE)],
            dst_ref=high.at[members],
            send_sem=halo_send.at[way],
            recv_sem=halo_recv.at[way, group],
            device_id={"seg": me, "freq": band - 1},
            device_id_type=MESH,
        )

    def forward(group):
        @pl.when(band < nfreq - 1)
        def _():
            upward(group).start()

        @pl.when(band > 0)
        def _():
            downward(group).start()

    def wait_halo(group):
        @pl.when(band < nfreq - 1)
        def _():
            downward(group).wait_recv()

        @pl.when(band > 0)
        def _():
            upward(group).wait_recv()

    barrier = pltpu.get_barrier_semaphore()

    @pl.when(inner)
    def _():
        for step in range(3 * size, 3 * size + PAIR):
            greet(step, barrier)
        for step in range(size, 2 * size):
            greet(step, barrier)
        pl.semaphore_wait(barrier, PAIR)
        for step in range(3 * size, 3 * size + PAIR):
            send_edge(step)
        for step in range(3 * size, 3 * size + PAIR):
            send_rest(step)

    @pl.when(outer)
    def _():
        greet_bands(barrier)
        pl.semaphore_wait(barrier, size + nfreq - 1)
        each(size, 2 * size, lambda step: greet(step, near_sem))
        greet_bands(band_sem)
        each(size, 2 * size, send_edge)
        each(size, size + PAIR, send_rest)

    own = pltpu.make_async_copy(
        coarse.at[:, pl.ds(pl.multiple_of(me * rows, rows), rows), :], maps.at[0], own_sem
    )
    own.start()
    load_shifts = pltpu.make_async_copy(offsets, shifts, shifts_sem)
    load_shifts.start()
    total[...] = jnp.zeros_like(total)

    @pl.when(band == 0)
    def _():
        low[...] = jnp.zeros_like(low)

    @pl.when(band == nfreq - 1)
    def _():
        high[...] = jnp.zeros_like(high)

    @pl.when(inner)
    def _():
        pl.semaphore_wait(near_sem, size)
        greet(3 * size, far_sem)
        each(size, 2 * size, send_edge)
        each(1, size, send_edge)
        each(1, 2 * size, send_rest)
        pl.semaphore_wait(far_sem, 1)
        greet(size, near_sem)
        each(3 * size + PAIR, nseg, send_edge)
        each(2 * size, 3 * size, send_edge)
        each(2 * size, 3 * size - PAIR, send_rest)
        send_parts(2)
        each(3 * size + PAIR, 4 * size - PAIR, send_rest)
        send_parts(3)
        if nfreq > 1:
            pl.semaphore_wait(band_sem, 1)

    @pl.when(outer)
    def _():
        if nfreq > 1:
            pl.semaphore_wait(band_sem, nfreq - 1)
            greet(size, band_sem)
        pl.semaphore_wait(near_sem, 1)
        each(2 * size, nseg, send_edge)
        each(1, size, send_edge)
        each(1, size, send_rest)
        each(size + PAIR, nseg, send_rest)

    def add(lines, best=None):
        lane = lax.broadcasted_iota(jnp.int32, (rows, EDGE), 1)
        columns = []
        for slot, (step, seg) in enumerate(lines):
            columns.append(partner(me, step, nseg) * local_segs + seg)
            ring = jnp.where(lane < EDGE // 2, high[step, seg], low[step, seg])
            line = jnp.concatenate([maps[step, seg], ring], axis=1)
            for shift in range(-HALO, HALO + 1):
                turned = line if shift == 0 else pltpu.roll(line, (-shift) % (bins + EDGE), 1)
                shifted[slot, HALO + shift] = turned[:, :bins]

        def spindown(spin, best):
            value = total[spin]
            for slot, column in enumerate(columns):
                value = value + shifted[slot, HALO + shifts[spin, column]]
            if best is not None:
                value = value * scale
                best = jnp.maximum(best, value)
            total[spin] = value
            return best

        return lax.fori_loop(0, spins, spindown, best, unroll=4)

    wait_edges(1, 0)
    forward(1)
    own.wait()
    wait_edges(0, 1)
    forward(0)
    wait_edges(3, 0)
    forward(3)
    wait_edges(2, 0)
    forward(2)
    load_shifts.wait()

    pairs = size // PAIR
    opens = 3 * pairs - 1
    wait_halo(0)
    wait_rest(1, PAIR - 1, local_segs, pair_recv.at[0])

    @pl.loop(0, 4 * pairs - 1)
    def _(turn):
        group = jnp.where(turn < 2 * pairs, turn // pairs, jnp.where(turn < opens, last_group, 5 - last_group))
        member = jnp.where(turn < opens, lax.rem(turn, pairs), turn - opens)
        pair = group * pairs + member

        @pl.when(jnp.logical_and(turn > 0, member == 0))
        def _():
            wait_halo(group)

        @pl.when(turn > 0)
        def _():
            wait_rest(PAIR, PAIR, local_segs, pair_recv.at[pair])

        @pl.loop(0, PAIR)
        def _(core):
            add([(pair * PAIR + core, seg) for seg in range(local_segs)])

    if pairs == 1:
        wait_halo(last_group)

    def lines_of(place):
        return [(last + core, begins[place] + seg) for core in range(PAIR) for seg in range(parts[place])]

    best = jnp.full((rows, bins), -jnp.inf, jnp.float32)
    for place, segs in enumerate(parts):
        wait_rest(PAIR, PAIR, segs, part_sem(last // PAIR, place))
        final = add(lines_of(place), best if place == len(parts) - 1 else None)
    best = final
    top = best[:, :EDGE]
    for begin in range(EDGE, bins, EDGE):
        top = jnp.maximum(top, best[:, begin : begin + EDGE])
    tops[0] = top

    def tell(step):
        return pltpu.make_async_remote_copy(
            src_ref=tops.at[0],
            dst_ref=tops.at[step],
            send_sem=top_send.at[step - 1],
            recv_sem=top_recv.at[step - 1],
            device_id={"seg": me, "freq": lax.rem(band + step, nfreq)},
            device_id_type=MESH,
        )

    for step in range(1, nfreq):
        tell(step).start()

    sent = coarse.at[:, pl.ds(0, (nseg - 1) * rows), :]
    wait_for(sent, send_sem)

    @pl.when(band < nfreq - 1)
    def _():
        wait_for(low, halo_send.at[0])

    @pl.when(band > 0)
    def _():
        wait_for(high, halo_send.at[halo_send.shape[0] - 1])

    for step in range(1, nfreq):
        tell(step).wait()
    top = tops[0]
    for step in range(1, nfreq):
        top = jnp.maximum(top, tops[step])
    total[spins, :, :EDGE] = top


def finish(total, fine, peaks, line, sem, line_sem):
    spins, rows = fine.shape[:2]
    write = pltpu.make_async_copy(total.at[pl.ds(0, spins)], fine, sem)
    write.start()
    row = lax.broadcasted_iota(jnp.int32, (rows, EDGE), 0)
    lane = lax.broadcasted_iota(jnp.int32, (rows, EDGE), 1)
    top = jnp.max(total[spins, :, :EDGE], axis=1, keepdims=True)
    line[...] = jnp.sum(jnp.where(row == lane, top, 0.0), axis=0)[:rows]
    write_line = pltpu.make_async_copy(line, peaks, line_sem)
    write_line.start()
    write.wait()
    write_line.wait()


def solution(mesh):
    nseg, nfreq = mesh.shape["seg"], mesh.shape["freq"]

    def on_device(coarse, offsets):
        local_segs, points, bins = coarse.shape
        rows = points // nseg
        spins = offsets.shape[1]
        parts = (local_segs - 2, 1, 1) if local_segs > 2 else (local_segs,)
        ways = 1 if nfreq <= 2 else 2
        hbm = pl.BlockSpec(memory_space=pltpu.HBM)
        vmem = pl.BlockSpec(memory_space=pltpu.VMEM)
        dma = pltpu.SemaphoreType.DMA
        signal = pltpu.SemaphoreType.REGULAR
        total = pl.pallas_call(
            functools.partial(kernel, nseg, nfreq, parts),
            out_shape=jax.ShapeDtypeStruct((spins + 1, rows, bins), jnp.float32),
            in_specs=[hbm, hbm],
            out_specs=vmem,
            scratch_shapes=[
                pltpu.VMEM((nseg, local_segs, rows, bins), jnp.float32),
                pltpu.VMEM((nseg, local_segs, rows, EDGE), jnp.float32),
                pltpu.VMEM((nseg, local_segs, rows, EDGE), jnp.float32),
                pltpu.VMEM((local_segs, SHIFTS, rows, bins), jnp.float32),
                pltpu.VMEM((nfreq, rows, EDGE), jnp.float32),
                pltpu.SMEM(offsets.shape[::-1], jnp.int32),
                dma,
                dma,
                dma,
                dma((PLANES,)),
                dma((nseg // PAIR,)),
                dma((max(len(parts) - 1, 1),)),
                dma((ways,)),
                dma((ways, PLANES)),
                dma((max(nfreq - 1, 1),)),
                dma((max(nfreq - 1, 1),)),
                signal,
                signal,
                signal,
            ],
            compiler_params=pltpu.CompilerParams(
                collective_id=0, has_side_effects=True, vmem_limit_bytes=32 << 20
            ),
        )(pltpu.with_memory_space_constraint(coarse, pltpu.HBM), pltpu.with_memory_space_constraint(offsets.T, pltpu.HBM))
        return pl.pallas_call(
            finish,
            out_shape=(
                jax.ShapeDtypeStruct((spins, rows, bins), jnp.float32),
                jax.ShapeDtypeStruct((rows,), jnp.float32),
            ),
            in_specs=[vmem],
            out_specs=(hbm, hbm),
            scratch_shapes=[pltpu.VMEM((rows,), jnp.float32), dma, dma],
            compiler_params=pltpu.CompilerParams(vmem_limit_bytes=8 << 20),
        )(total)

    return jax.shard_map(
        on_device,
        mesh=mesh,
        in_specs=(P("seg", None, "freq"), P()),
        out_specs=(P(None, "seg", "freq"), P("seg")),
        check_vma=False,
    )
```

```python
import functools

import jax
import jax.numpy as jnp
from jax import lax
from jax.experimental import pallas as pl
from jax.experimental.pallas import tpu as pltpu
from jax.sharding import PartitionSpec as P

HALO = 8
EDGE = 128
SHIFTS = 2 * HALO + 1
PLANES = 4
PAIR = 2
ORDER = (
    ("part", 0, 0),
    ("part", 0, 1),
    ("part", 1, 0),
    ("part", 1, 1),
    ("part", 2, 0),
    ("part", 2, 1),
    ("tail", 0),
    ("tail", 1),
)
MESH = pl.DeviceIdType.MESH


def partner(me, step, count):
    result = me
    bit = 1
    while bit < count:
        wanted = (step // bit) % 2 if isinstance(step, int) else lax.rem(step // bit, 2)
        held = lax.rem(me // bit, 2)
        result = result + bit * wanted * (1 - 2 * held)
        bit *= 2
    return result


def kernel(
    nseg,
    nfreq,
    parts,
    coarse,
    offsets,
    total,
    maps,
    low,
    high,
    shifted,
    tops,
    shifts,
    own_sem,
    shifts_sem,
    send_sem,
    edge_recv,
    pair_recv,
    part_recv,
    tail_recv,
    halo_send,
    halo_recv,
    top_send,
    top_recv,
    near_sem,
    far_sem,
    band_sem,
):
    local_segs = coarse.shape[0]
    spins = total.shape[0] - 1
    rows, bins = total.shape[1:]
    scale = 1.0 / (nseg * local_segs)
    size = nseg // PLANES
    begins = [sum(parts[:place]) for place in range(len(parts))]
    bulk = local_segs - 1
    me = lax.axis_index("seg")
    band = lax.axis_index("freq")
    plane = me // size
    inner = lax.rem((plane + 1) // 2, 2) == 1
    outer = jnp.logical_not(inner)
    last_group = jnp.where(inner, 3, 2)
    last = (last_group + 1) * size - PAIR

    early = EDGE if nfreq <= 2 else bins
    width = bins - early
    edge_at = jnp.where(band == 0, bins - early, 0)
    rest_at = jnp.where(band == 0, 0, early)

    def each(begin, end, act):
        @pl.loop(begin, end)
        def _(step):
            act(step)

    def greet(step, sem):
        pl.semaphore_signal(
            sem, inc=1, device_id={"seg": partner(me, step, nseg), "freq": band}, device_id_type=MESH
        )

    def greet_bands(sem):
        for step in range(1, nfreq):
            pl.semaphore_signal(
                sem, inc=1, device_id={"seg": me, "freq": lax.rem(band + step, nfreq)}, device_id_type=MESH
            )

    def send(step, begin, count, first, segs, received):
        other = partner(me, step, nseg)
        columns = pl.ds(pl.multiple_of(begin, EDGE), count)
        rows_of = pl.ds(pl.multiple_of(other * rows, rows), rows)
        members = pl.ds(first, segs)
        pltpu.make_async_remote_copy(
            src_ref=coarse.at[members, rows_of, columns],
            dst_ref=maps.at[step, members, :, columns],
            send_sem=send_sem,
            recv_sem=received,
            device_id={"seg": other, "freq": band},
            device_id_type=MESH,
        ).start()

    def send_edge(step):
        send(step, edge_at, early, 0, local_segs, edge_recv.at[step // size])

    def send_rest(step):
        if width:
            send(step, rest_at, width, 0, local_segs, pair_recv.at[step // PAIR])

    def part_sem(pair, place):
        return part_recv.at[place - 1] if place else pair_recv.at[pair]

    def send_bulk(step):
        if width:
            send(step, rest_at, width, 0, bulk, pair_recv.at[step // PAIR])

    def send_ends(group):
        first = (group + 1) * size - PAIR
        lead = group * size

        def part(place, core):
            step = first + lax.rem(lax.rem(me, PAIR) + core, PAIR)
            send(step, rest_at, width, begins[place], parts[place], part_sem(first // PAIR, place))

        def tail(core):
            step = lead + lax.rem(lax.rem(me, PAIR) + core, PAIR)
            send(step, rest_at, width, bulk, 1, tail_recv)

        if width:
            for act, *args in ORDER:
                (part if act == "part" else tail)(*args)

    def wait_for(there, sem):
        pltpu.make_async_copy(there, there, sem).wait()

    def wait_edges(group, first):
        wait_for(maps.at[pl.ds(group * size + first, size - first), :, :, pl.ds(0, early)], edge_recv.at[group])

    def wait_rest(step, steps, segs, sem):
        if width:
            wait_for(maps.at[pl.ds(step, steps), pl.ds(0, segs), :, pl.ds(0, width)], sem)

    def upward(group):
        members = pl.ds(group * size, size)
        return pltpu.make_async_remote_copy(
            src_ref=maps.at[members, :, :, pl.ds(bins - EDGE, EDGE)],
            dst_ref=low.at[members],
            send_sem=halo_send.at[0],
            recv_sem=halo_recv.at[0, group],
            device_id={"seg": me, "freq": band + 1},
            device_id_type=MESH,
        )

    def downward(group):
        members = pl.ds(group * size, size)
        way = halo_send.shape[0] - 1
        return pltpu.make_async_remote_copy(
            src_ref=maps.at[members, :, :, pl.ds(0, EDGE)],
            dst_ref=high.at[members],
            send_sem=halo_send.at[way],
            recv_sem=halo_recv.at[way, group],
            device_id={"seg": me, "freq": band - 1},
            device_id_type=MESH,
        )

    def forward(group):
        @pl.when(band < nfreq - 1)
        def _():
            upward(group).start()

        @pl.when(band > 0)
        def _():
            downward(group).start()

    def wait_halo(group):
        @pl.when(band < nfreq - 1)
        def _():
            downward(group).wait_recv()

        @pl.when(band > 0)
        def _():
            upward(group).wait_recv()

    barrier = pltpu.get_barrier_semaphore()

    @pl.when(inner)
    def _():
        for step in range(3 * size, 3 * size + PAIR):
            greet(step, barrier)
        for step in range(size, 2 * size):
            greet(step, barrier)
        pl.semaphore_wait(barrier, PAIR)
        for step in range(3 * size, 3 * size + PAIR):
            send_edge(step)
        for step in range(3 * size, 3 * size + PAIR):
            send_bulk(step)

    @pl.when(outer)
    def _():
        greet_bands(barrier)
        pl.semaphore_wait(barrier, size + nfreq - 1)
        each(size, 2 * size, lambda step: greet(step, near_sem))
        greet_bands(band_sem)
        each(size, 2 * size, send_edge)
        each(size, size + PAIR, send_rest)

    own = pltpu.make_async_copy(
        coarse.at[:, pl.ds(pl.multiple_of(me * rows, rows), rows), :], maps.at[0], own_sem
    )
    own.start()
    load_shifts = pltpu.make_async_copy(offsets, shifts, shifts_sem)
    load_shifts.start()
    total[...] = jnp.zeros_like(total)

    @pl.when(band == 0)
    def _():
        low[...] = jnp.zeros_like(low)

    @pl.when(band == nfreq - 1)
    def _():
        high[...] = jnp.zeros_like(high)

    @pl.when(inner)
    def _():
        pl.semaphore_wait(near_sem, size)
        greet(3 * size, far_sem)
        pl.semaphore_wait(far_sem, 1)
        greet(size, near_sem)
        each(3 * size + PAIR, nseg, send_edge)
        each(2 * size, 3 * size, send_edge)
        each(size, 2 * size, send_edge)
        each(1, size, send_edge)
        each(1, 2 * size, send_rest)
        each(2 * size, 2 * size + PAIR, send_bulk)
        each(2 * size + PAIR, 3 * size - PAIR, send_rest)
        send_ends(2)
        each(3 * size + PAIR, 4 * size - PAIR, send_rest)
        send_ends(3)
        if nfreq > 1:
            pl.semaphore_wait(band_sem, 1)

    @pl.when(outer)
    def _():
        if nfreq > 1:
            pl.semaphore_wait(band_sem, nfreq - 1)
            greet(size, band_sem)
        pl.semaphore_wait(near_sem, 1)
        each(2 * size, nseg, send_edge)
        each(1, size, send_edge)
        each(1, size, send_rest)
        each(size + PAIR, nseg, send_rest)

    lane = lax.broadcasted_iota(jnp.int32, (rows, EDGE), 1)

    def column_of(step, seg):
        return partner(me, step, nseg) * local_segs + seg

    def line_of(step, seg):
        ring = jnp.where(lane < EDGE // 2, high[step, seg], low[step, seg])
        return jnp.concatenate([maps[step, seg], ring], axis=1)

    def add(lines, best=None):
        columns = [column_of(step, seg) for step, seg in lines]
        for slot, (step, seg) in enumerate(lines):
            line = line_of(step, seg)
            for shift in range(-HALO, HALO + 1):
                turned = line if shift == 0 else pltpu.roll(line, (-shift) % (bins + EDGE), 1)
                shifted[slot, HALO + shift] = turned[:, :bins]

        def spindown(spin, best):
            value = total[spin]
            for slot, column in enumerate(columns):
                value = value + shifted[slot, HALO + shifts[spin, column]]
            if best is not None:
                value = value * scale
                best = jnp.maximum(best, value)
            total[spin] = value
            return best

        return lax.fori_loop(0, spins, spindown, best, unroll=4 if len(lines) > PAIR else 8)

    wait_edges(1, 0)
    forward(1)
    own.wait()
    wait_edges(0, 1)
    forward(0)
    wait_edges(3, 0)
    forward(3)
    wait_edges(2, 0)
    forward(2)
    load_shifts.wait()

    pairs = size // PAIR
    opens = 3 * pairs - 1
    wait_halo(0)
    wait_rest(1, PAIR - 1, local_segs, pair_recv.at[0])

    @pl.loop(0, 4 * pairs - 1)
    def _(turn):
        group = jnp.where(turn < 2 * pairs, turn // pairs, jnp.where(turn < opens, last_group, 5 - last_group))
        member = jnp.where(turn < opens, lax.rem(turn, pairs), turn - opens)
        pair = group * pairs + member

        @pl.when(jnp.logical_and(turn > 0, member == 0))
        def _():
            wait_halo(group)

        def take(segs, waits):
            @pl.when(waits)
            def _():
                wait_rest(PAIR, PAIR, segs, pair_recv.at[pair])

            @pl.loop(0, PAIR)
            def _(core):
                add([(pair * PAIR + core, seg) for seg in range(segs)])

        @pl.when(turn != 2 * pairs)
        def _():
            take(local_segs, turn > 0)

        @pl.when(turn == 2 * pairs)
        def _():
            take(bulk, True)

    def lines_of(place):
        return [(last + core, begins[place] + seg) for core in range(PAIR) for seg in range(parts[place])]

    for place, segs in enumerate(parts):
        wait_rest(PAIR, PAIR, segs, part_sem(last // PAIR, place))
        add(lines_of(place))
    wait_rest(PAIR, PAIR, 1, tail_recv)
    best = add(
        [(last_group * size + core, bulk) for core in range(PAIR)], jnp.full((rows, bins), -jnp.inf, jnp.float32)
    )
    top = best[:, :EDGE]
    for begin in range(EDGE, bins, EDGE):
        top = jnp.maximum(top, best[:, begin : begin + EDGE])
    tops[0] = top

    def tell(step):
        return pltpu.make_async_remote_copy(
            src_ref=tops.at[0],
            dst_ref=tops.at[step],
            send_sem=top_send.at[step - 1],
            recv_sem=top_recv.at[step - 1],
            device_id={"seg": me, "freq": lax.rem(band + step, nfreq)},
            device_id_type=MESH,
        )

    for step in range(1, nfreq):
        tell(step).start()

    sent = coarse.at[:, pl.ds(0, (nseg - 1) * rows), :]
    wait_for(sent, send_sem)

    @pl.when(band < nfreq - 1)
    def _():
        wait_for(low, halo_send.at[0])

    @pl.when(band > 0)
    def _():
        wait_for(high, halo_send.at[halo_send.shape[0] - 1])

    for step in range(1, nfreq):
        tell(step).wait()
    top = tops[0]
    for step in range(1, nfreq):
        top = jnp.maximum(top, tops[step])
    total[spins, :, :EDGE] = top


def finish(total, fine, peaks, line, sem, line_sem):
    spins, rows = fine.shape[:2]
    write = pltpu.make_async_copy(total.at[pl.ds(0, spins)], fine, sem)
    write.start()
    row = lax.broadcasted_iota(jnp.int32, (rows, EDGE), 0)
    lane = lax.broadcasted_iota(jnp.int32, (rows, EDGE), 1)
    top = jnp.max(total[spins, :, :EDGE], axis=1, keepdims=True)
    line[...] = jnp.sum(jnp.where(row == lane, top, 0.0), axis=0)[:rows]
    write_line = pltpu.make_async_copy(line, peaks, line_sem)
    write_line.start()
    write.wait()
    write_line.wait()


def solution(mesh):
    nseg, nfreq = mesh.shape["seg"], mesh.shape["freq"]

    def on_device(coarse, offsets):
        local_segs, points, bins = coarse.shape
        rows = points // nseg
        spins = offsets.shape[1]
        parts = (local_segs - 2, 1, 1)
        ways = 1 if nfreq <= 2 else 2
        hbm = pl.BlockSpec(memory_space=pltpu.HBM)
        vmem = pl.BlockSpec(memory_space=pltpu.VMEM)
        dma = pltpu.SemaphoreType.DMA
        signal = pltpu.SemaphoreType.REGULAR
        total = pl.pallas_call(
            functools.partial(kernel, nseg, nfreq, parts),
            out_shape=jax.ShapeDtypeStruct((spins + 1, rows, bins), jnp.float32),
            in_specs=[hbm, hbm],
            out_specs=vmem,
            scratch_shapes=[
                pltpu.VMEM((nseg, local_segs, rows, bins), jnp.float32),
                pltpu.VMEM((nseg, local_segs, rows, EDGE), jnp.float32),
                pltpu.VMEM((nseg, local_segs, rows, EDGE), jnp.float32),
                pltpu.VMEM((local_segs, SHIFTS, rows, bins), jnp.float32),
                pltpu.VMEM((nfreq, rows, EDGE), jnp.float32),
                pltpu.SMEM(offsets.shape[::-1], jnp.int32),
                dma,
                dma,
                dma,
                dma((PLANES,)),
                dma((nseg // PAIR,)),
                dma((len(parts) - 1,)),
                dma,
                dma((ways,)),
                dma((ways, PLANES)),
                dma((max(nfreq - 1, 1),)),
                dma((max(nfreq - 1, 1),)),
                signal,
                signal,
                signal,
            ],
            compiler_params=pltpu.CompilerParams(
                collective_id=0, has_side_effects=True, vmem_limit_bytes=32 << 20
            ),
        )(pltpu.with_memory_space_constraint(coarse, pltpu.HBM), pltpu.with_memory_space_constraint(offsets.T, pltpu.HBM))
        return pl.pallas_call(
            finish,
            out_shape=(
                jax.ShapeDtypeStruct((spins, rows, bins), jnp.float32),
                jax.ShapeDtypeStruct((rows,), jnp.float32),
            ),
            in_specs=[vmem],
            out_specs=(hbm, hbm),
            scratch_shapes=[pltpu.VMEM((rows,), jnp.float32), dma, dma],
            compiler_params=pltpu.CompilerParams(vmem_limit_bytes=8 << 20),
        )(total)

    return jax.shard_map(
        on_device,
        mesh=mesh,
        in_specs=(P("seg", None, "freq"), P()),
        out_specs=(P(None, "seg", "freq"), P("seg")),
        check_vma=False,
    )
```

```python
import functools

import jax
import jax.numpy as jnp
from jax import lax
from jax.experimental import pallas as pl
from jax.experimental.pallas import tpu as pltpu
from jax.sharding import PartitionSpec as P

HALO = 8
EDGE = 128
SHIFTS = 2 * HALO + 1
PLANES = 4
PAIR = 2
ORDER = (
    ("part", 0, 0),
    ("part", 0, 1),
    ("part", 1, 0),
    ("part", 2, 0),
    ("part", 1, 1),
    ("part", 2, 1),
    ("tail", 0),
    ("tail", 1),
)
CHUNK = EDGE // 2
MESH = pl.DeviceIdType.MESH


def partner(me, step, count):
    result = me
    bit = 1
    while bit < count:
        wanted = (step // bit) % 2 if isinstance(step, int) else lax.rem(step // bit, 2)
        held = lax.rem(me // bit, 2)
        result = result + bit * wanted * (1 - 2 * held)
        bit *= 2
    return result


def kernel(
    nseg,
    nfreq,
    parts,
    coarse,
    offsets,
    total,
    maps,
    low,
    high,
    shifted,
    turned,
    chunks,
    tops,
    shifts,
    own_sem,
    shifts_sem,
    send_sem,
    edge_recv,
    pair_recv,
    part_recv,
    tail_recv,
    halo_send,
    halo_recv,
    top_send,
    top_recv,
    near_sem,
    far_sem,
    band_sem,
):
    local_segs = coarse.shape[0]
    spins = total.shape[0] - 1
    rows, bins = total.shape[1:]
    scale = 1.0 / (nseg * local_segs)
    size = nseg // PLANES
    begins = [sum(parts[:place]) for place in range(len(parts))]
    bulk = local_segs - 1
    me = lax.axis_index("seg")
    band = lax.axis_index("freq")
    plane = me // size
    inner = lax.rem((plane + 1) // 2, 2) == 1
    outer = jnp.logical_not(inner)
    last_group = jnp.where(inner, 3, 2)
    last = (last_group + 1) * size - PAIR

    early = EDGE if nfreq <= 2 else bins
    width = bins - early
    edge_at = jnp.where(band == 0, bins - early, 0)
    rest_at = jnp.where(band == 0, 0, early)

    def each(begin, end, act):
        @pl.loop(begin, end)
        def _(step):
            act(step)

    def greet(step, sem):
        pl.semaphore_signal(
            sem, inc=1, device_id={"seg": partner(me, step, nseg), "freq": band}, device_id_type=MESH
        )

    def greet_bands(sem):
        for step in range(1, nfreq):
            pl.semaphore_signal(
                sem, inc=1, device_id={"seg": me, "freq": lax.rem(band + step, nfreq)}, device_id_type=MESH
            )

    def send(step, begin, count, first, segs, received):
        other = partner(me, step, nseg)
        columns = pl.ds(pl.multiple_of(begin, EDGE), count)
        rows_of = pl.ds(pl.multiple_of(other * rows, rows), rows)
        members = pl.ds(first, segs)
        pltpu.make_async_remote_copy(
            src_ref=coarse.at[members, rows_of, columns],
            dst_ref=maps.at[step, members, :, columns],
            send_sem=send_sem,
            recv_sem=received,
            device_id={"seg": other, "freq": band},
            device_id_type=MESH,
        ).start()

    def send_edge(step):
        send(step, edge_at, early, 0, local_segs, edge_recv.at[step // size])

    def send_rest(step):
        if width:
            send(step, rest_at, width, 0, local_segs, pair_recv.at[step // PAIR])

    def part_sem(pair, place):
        return part_recv.at[place - 1] if place else pair_recv.at[pair]

    def send_bulk(step):
        if width:
            send(step, rest_at, width, 0, bulk, pair_recv.at[step // PAIR])

    def send_ends(group):
        first = (group + 1) * size - PAIR
        lead = group * size

        def part(place, core):
            step = first + lax.rem(lax.rem(me, PAIR) + core, PAIR)
            send(step, rest_at, width, begins[place], parts[place], part_sem(first // PAIR, place))

        def tail(core):
            step = lead + lax.rem(lax.rem(me, PAIR) + core, PAIR)
            send(step, rest_at, width, bulk, 1, tail_recv)

        if width:
            for act, *args in ORDER:
                (part if act == "part" else tail)(*args)

    def wait_for(there, sem):
        pltpu.make_async_copy(there, there, sem).wait()

    def wait_edges(group, first):
        wait_for(maps.at[pl.ds(group * size + first, size - first), :, :, pl.ds(0, early)], edge_recv.at[group])

    def wait_rest(step, steps, segs, sem):
        if width:
            wait_for(maps.at[pl.ds(step, steps), pl.ds(0, segs), :, pl.ds(0, width)], sem)

    def upward(group):
        members = pl.ds(group * size, size)
        return pltpu.make_async_remote_copy(
            src_ref=maps.at[members, :, :, pl.ds(bins - EDGE, EDGE)],
            dst_ref=low.at[members],
            send_sem=halo_send.at[0],
            recv_sem=halo_recv.at[0, group],
            device_id={"seg": me, "freq": band + 1},
            device_id_type=MESH,
        )

    def downward(group):
        members = pl.ds(group * size, size)
        way = halo_send.shape[0] - 1
        return pltpu.make_async_remote_copy(
            src_ref=maps.at[members, :, :, pl.ds(0, EDGE)],
            dst_ref=high.at[members],
            send_sem=halo_send.at[way],
            recv_sem=halo_recv.at[way, group],
            device_id={"seg": me, "freq": band - 1},
            device_id_type=MESH,
        )

    def forward(group):
        @pl.when(band < nfreq - 1)
        def _():
            upward(group).start()

        @pl.when(band > 0)
        def _():
            downward(group).start()

    def wait_halo(group):
        @pl.when(band < nfreq - 1)
        def _():
            downward(group).wait_recv()

        @pl.when(band > 0)
        def _():
            upward(group).wait_recv()

    barrier = pltpu.get_barrier_semaphore()

    @pl.when(inner)
    def _():
        for step in range(3 * size, 3 * size + PAIR):
            greet(step, barrier)
        for step in range(size, 2 * size):
            greet(step, barrier)
        pl.semaphore_wait(barrier, PAIR)
        for step in range(3 * size, 3 * size + PAIR):
            send_edge(step)
        for step in range(3 * size, 3 * size + PAIR):
            send_bulk(step)

    @pl.when(outer)
    def _():
        greet_bands(barrier)
        pl.semaphore_wait(barrier, size + nfreq - 1)
        each(size, 2 * size, lambda step: greet(step, near_sem))
        greet_bands(band_sem)
        each(size, 2 * size, send_edge)
        each(size, size + PAIR, send_rest)

    own = pltpu.make_async_copy(
        coarse.at[:, pl.ds(pl.multiple_of(me * rows, rows), rows), :], maps.at[0], own_sem
    )
    own.start()
    load_shifts = pltpu.make_async_copy(offsets, shifts, shifts_sem)
    load_shifts.start()
    total[...] = jnp.zeros_like(total)

    @pl.when(band == 0)
    def _():
        low[...] = jnp.zeros_like(low)

    @pl.when(band == nfreq - 1)
    def _():
        high[...] = jnp.zeros_like(high)

    @pl.when(inner)
    def _():
        pl.semaphore_wait(near_sem, size)
        greet(3 * size, far_sem)
        pl.semaphore_wait(far_sem, 1)
        greet(size, near_sem)
        each(3 * size + PAIR, nseg, send_edge)
        each(2 * size, 3 * size, send_edge)
        each(size, 2 * size, send_edge)
        each(1, size, send_edge)
        each(1, 2 * size, send_rest)
        each(2 * size, 2 * size + PAIR, send_bulk)
        each(2 * size + PAIR, 3 * size - PAIR, send_rest)
        send_ends(2)
        each(3 * size + PAIR, 4 * size - PAIR, send_rest)
        send_ends(3)
        if nfreq > 1:
            pl.semaphore_wait(band_sem, 1)

    @pl.when(outer)
    def _():
        if nfreq > 1:
            pl.semaphore_wait(band_sem, nfreq - 1)
            greet(size, band_sem)
        pl.semaphore_wait(near_sem, 1)
        each(2 * size, nseg, send_edge)
        each(1, size, send_edge)
        each(1, size, send_rest)
        each(size + PAIR, nseg, send_rest)

    lane = lax.broadcasted_iota(jnp.int32, (rows, EDGE), 1)

    def column_of(step, seg):
        return partner(me, step, nseg) * local_segs + seg

    def ring_of(step, seg):
        return jnp.where(lane < EDGE // 2, high[step, seg], low[step, seg])

    def add(lines):
        columns = [column_of(step, seg) for step, seg in lines]
        for slot, (step, seg) in enumerate(lines):
            line = jnp.concatenate([maps[step, seg], ring_of(step, seg)], axis=1)
            for shift in range(-HALO, HALO + 1):
                turned_line = line if shift == 0 else pltpu.roll(line, (-shift) % (bins + EDGE), 1)
                shifted[slot, HALO + shift] = turned_line[:, :bins]

        @pl.loop(0, spins, unroll=4)
        def _(spin):
            value = total[spin]
            for slot, column in enumerate(columns):
                value = value + shifted[slot, HALO + shifts[spin, column]]
            total[spin] = value

    tiles = bins // EDGE
    first_half = lane < CHUNK

    def turn_totals():
        @pl.loop(0, spins // 2, unroll=8)
        def _(pair):
            blocks = []
            for at in range(0, bins, EDGE):
                one = total[2 * pair, :, at : at + EDGE]
                two = total[2 * pair + 1, :, at : at + EDGE]
                blocks.append(jnp.where(first_half, one, pltpu.roll(two, CHUNK, 1)))
                blocks.append(jnp.where(first_half, pltpu.roll(one, CHUNK, 1), two))
            square = jnp.concatenate(blocks, axis=0).T
            turned[2 * pair] = square[:CHUNK]
            turned[2 * pair + 1] = square[CHUNK:]

    def turn_back():
        @pl.loop(0, spins // 2, unroll=8)
        def _(pair):
            square = jnp.concatenate([turned[2 * pair], turned[2 * pair + 1]], axis=0).T
            for tile in range(tiles):
                at = tile * EDGE
                even = square[2 * tile * rows : (2 * tile + 1) * rows]
                odd = square[(2 * tile + 1) * rows : (2 * tile + 2) * rows]
                total[2 * pair, :, at : at + EDGE] = jnp.where(first_half, even, pltpu.roll(odd, CHUNK, 1))
                total[2 * pair + 1, :, at : at + EDGE] = jnp.where(first_half, pltpu.roll(even, CHUNK, 1), odd)

    def add_turned(lines, best=None):
        columns = [column_of(step, seg) for step, seg in lines]
        own_half = lane < CHUNK + CHUNK // 2
        next_part = jnp.logical_and(lane >= CHUNK, own_half)
        for slot, (step, seg) in enumerate(lines):
            whole = [maps[step, seg, :, at : at + EDGE] for at in range(0, bins, EDGE)] + [ring_of(step, seg)]
            half = [pltpu.roll(tile, CHUNK, 1) for tile in whole]
            blocks = []
            for tile in range(tiles):
                blocks.append(jnp.where(own_half, whole[tile], whole[tile - 1]))
                blocks.append(jnp.where(next_part, half[tile + 1], half[tile]))
            square = jnp.concatenate(blocks, axis=0).T
            chunks[slot, :HALO] = square[EDGE - HALO :]
            chunks[slot, HALO:] = square[: CHUNK + HALO]

        def spindown(spin, best):
            value = turned[spin]
            for slot, column in enumerate(columns):
                value = value + chunks[slot, pl.ds(HALO + shifts[spin, column], CHUNK)]
            if best is not None:
                value = value * scale
                best = jnp.maximum(best, value)
            turned[spin] = value
            return best

        return lax.fori_loop(0, spins, spindown, best, unroll=8)

    wait_edges(1, 0)
    forward(1)
    own.wait()
    wait_edges(0, 1)
    forward(0)
    wait_edges(3, 0)
    forward(3)
    wait_edges(2, 0)
    forward(2)
    load_shifts.wait()

    pairs = size // PAIR
    opens = 3 * pairs - 1
    wait_halo(0)
    wait_rest(1, PAIR - 1, local_segs, pair_recv.at[0])

    @pl.loop(0, 4 * pairs - 1)
    def _(turn):
        group = jnp.where(turn < 2 * pairs, turn // pairs, jnp.where(turn < opens, last_group, 5 - last_group))
        member = jnp.where(turn < opens, lax.rem(turn, pairs), turn - opens)
        pair = group * pairs + member

        @pl.when(jnp.logical_and(turn > 0, member == 0))
        def _():
            wait_halo(group)

        def take(segs, waits):
            @pl.when(waits)
            def _():
                wait_rest(PAIR, PAIR, segs, pair_recv.at[pair])

            @pl.loop(0, PAIR)
            def _(core):
                add([(pair * PAIR + core, seg) for seg in range(segs)])

        @pl.when(turn != 2 * pairs)
        def _():
            take(local_segs, turn > 0)

        @pl.when(turn == 2 * pairs)
        def _():
            take(bulk, True)

    def lines_of(place):
        return [(last + core, begins[place] + seg) for core in range(PAIR) for seg in range(parts[place])]

    turn_totals()
    for place, segs in enumerate(parts):
        wait_rest(PAIR, PAIR, segs, part_sem(last // PAIR, place))
        add_turned(lines_of(place))
    wait_rest(PAIR, PAIR, 1, tail_recv)
    best = add_turned(
        [(last_group * size + core, bulk) for core in range(PAIR)], jnp.full((CHUNK, EDGE), -jnp.inf, jnp.float32)
    )
    top = best[:rows]
    for begin in range(rows, CHUNK, rows):
        top = jnp.maximum(top, best[begin : begin + rows])
    tops[0] = top

    def tell(step):
        return pltpu.make_async_remote_copy(
            src_ref=tops.at[0],
            dst_ref=tops.at[step],
            send_sem=top_send.at[step - 1],
            recv_sem=top_recv.at[step - 1],
            device_id={"seg": me, "freq": lax.rem(band + step, nfreq)},
            device_id_type=MESH,
        )

    for step in range(1, nfreq):
        tell(step).start()

    turn_back()
    sent = coarse.at[:, pl.ds(0, (nseg - 1) * rows), :]
    wait_for(sent, send_sem)

    @pl.when(band < nfreq - 1)
    def _():
        wait_for(low, halo_send.at[0])

    @pl.when(band > 0)
    def _():
        wait_for(high, halo_send.at[halo_send.shape[0] - 1])

    for step in range(1, nfreq):
        tell(step).wait()
    top = tops[0]
    for step in range(1, nfreq):
        top = jnp.maximum(top, tops[step])
    total[spins, :, :EDGE] = top


def finish(total, fine, peaks, line, sem, line_sem):
    spins, rows = fine.shape[:2]
    write = pltpu.make_async_copy(total.at[pl.ds(0, spins)], fine, sem)
    write.start()
    top = jnp.max(total[spins, :, :EDGE], axis=0, keepdims=True)
    apart = EDGE // 2
    while apart >= rows:
        top = jnp.maximum(top, pltpu.roll(top, apart, 1))
        apart //= 2
    line[...] = top[0, :rows]
    write_line = pltpu.make_async_copy(line, peaks, line_sem)
    write_line.start()
    write.wait()
    write_line.wait()


def solution(mesh):
    nseg, nfreq = mesh.shape["seg"], mesh.shape["freq"]

    def on_device(coarse, offsets):
        local_segs, points, bins = coarse.shape
        rows = points // nseg
        spins = offsets.shape[1]
        parts = (local_segs - 2, 1, 1)
        ways = 1 if nfreq <= 2 else 2
        if rows * bins != EDGE * CHUNK or nseg % (2 * PAIR * PLANES) or spins % 2:
            raise ValueError("unsupported shape")
        hbm = pl.BlockSpec(memory_space=pltpu.HBM)
        vmem = pl.BlockSpec(memory_space=pltpu.VMEM)
        dma = pltpu.SemaphoreType.DMA
        signal = pltpu.SemaphoreType.REGULAR
        total = pl.pallas_call(
            functools.partial(kernel, nseg, nfreq, parts),
            out_shape=jax.ShapeDtypeStruct((spins + 1, rows, bins), jnp.float32),
            in_specs=[hbm, hbm],
            out_specs=vmem,
            scratch_shapes=[
                pltpu.VMEM((nseg, local_segs, rows, bins), jnp.float32),
                pltpu.VMEM((nseg, local_segs, rows, EDGE), jnp.float32),
                pltpu.VMEM((nseg, local_segs, rows, EDGE), jnp.float32),
                pltpu.VMEM((local_segs, SHIFTS, rows, bins), jnp.float32),
                pltpu.VMEM((spins, CHUNK, EDGE), jnp.float32),
                pltpu.VMEM((PAIR * max(parts), CHUNK + 2 * HALO, EDGE), jnp.float32),
                pltpu.VMEM((nfreq, rows, EDGE), jnp.float32),
                pltpu.SMEM(offsets.shape[::-1], jnp.int32),
                dma,
                dma,
                dma,
                dma((PLANES,)),
                dma((nseg // PAIR,)),
                dma((len(parts) - 1,)),
                dma,
                dma((ways,)),
                dma((ways, PLANES)),
                dma((max(nfreq - 1, 1),)),
                dma((max(nfreq - 1, 1),)),
                signal,
                signal,
                signal,
            ],
            compiler_params=pltpu.CompilerParams(
                collective_id=0, has_side_effects=True, vmem_limit_bytes=32 << 20
            ),
        )(pltpu.with_memory_space_constraint(coarse, pltpu.HBM), pltpu.with_memory_space_constraint(offsets.T, pltpu.HBM))
        return pl.pallas_call(
            finish,
            out_shape=(
                jax.ShapeDtypeStruct((spins, rows, bins), jnp.float32),
                jax.ShapeDtypeStruct((rows,), jnp.float32),
            ),
            in_specs=[vmem],
            out_specs=(hbm, hbm),
            scratch_shapes=[pltpu.VMEM((rows,), jnp.float32), dma, dma],
            compiler_params=pltpu.CompilerParams(vmem_limit_bytes=8 << 20),
        )(total)

    return jax.shard_map(
        on_device,
        mesh=mesh,
        in_specs=(P("seg", None, "freq"), P()),
        out_specs=(P(None, "seg", "freq"), P("seg")),
        check_vma=False,
    )
```

```python
import functools

import jax
import jax.numpy as jnp
from jax import lax
from jax.experimental import pallas as pl
from jax.experimental.pallas import tpu as pltpu
from jax.sharding import PartitionSpec as P

HALO = 8
EDGE = 128
SHIFTS = 2 * HALO + 1
PLANES = 4
PAIR = 2
ORDER = (
    ("part", 0, 0),
    ("part", 0, 1),
    ("part", 1, 0),
    ("part", 2, 0),
    ("part", 1, 1),
    ("part", 2, 1),
    ("tail", 1, 0),
    ("tail", 2, 1),
    ("tail", 1, 1),
)
TAILS = (1, 2)
PASSED = 5
CHUNK = EDGE // 2
MESH = pl.DeviceIdType.MESH


def partner(me, step, count):
    result = me
    bit = 1
    while bit < count:
        wanted = (step // bit) % 2 if isinstance(step, int) else lax.rem(step // bit, 2)
        held = lax.rem(me // bit, 2)
        result = result + bit * wanted * (1 - 2 * held)
        bit *= 2
    return result


def kernel(
    nseg,
    nfreq,
    parts,
    coarse,
    offsets,
    total,
    maps,
    low,
    high,
    shifted,
    turned,
    chunks,
    passed,
    tops,
    shifts,
    own_sem,
    shifts_sem,
    send_sem,
    edge_recv,
    pair_recv,
    part_recv,
    tail_recv,
    halo_send,
    halo_recv,
    top_send,
    top_recv,
    near_sem,
    far_sem,
    band_sem,
    pass_send,
    pass_recv,
):
    local_segs = coarse.shape[0]
    spins = total.shape[0] - 1
    rows, bins = total.shape[1:]
    scale = 1.0 / (nseg * local_segs)
    size = nseg // PLANES
    begins = [sum(parts[:place]) for place in range(len(parts))]
    me = lax.axis_index("seg")
    core = lax.rem(me, PAIR)
    band = lax.axis_index("freq")
    plane = me // size
    inner = lax.rem((plane + 1) // 2, 2) == 1
    outer = jnp.logical_not(inner)
    last_group = jnp.where(inner, 3, 2)
    last = (last_group + 1) * size - PAIR

    early = EDGE if nfreq <= 2 else bins
    width = bins - early
    edge_at = jnp.where(band == 0, bins - early, 0)
    rest_at = jnp.where(band == 0, 0, early)

    def each(begin, end, act):
        @pl.loop(begin, end)
        def _(step):
            act(step)

    def greet(step, sem):
        pl.semaphore_signal(
            sem, inc=1, device_id={"seg": partner(me, step, nseg), "freq": band}, device_id_type=MESH
        )

    def greet_bands(sem):
        for step in range(1, nfreq):
            pl.semaphore_signal(
                sem, inc=1, device_id={"seg": me, "freq": lax.rem(band + step, nfreq)}, device_id_type=MESH
            )

    def send(step, begin, count, first, segs, received):
        other = partner(me, step, nseg)
        columns = pl.ds(pl.multiple_of(begin, EDGE), count)
        rows_of = pl.ds(pl.multiple_of(other * rows, rows), rows)
        members = pl.ds(first, segs)
        pltpu.make_async_remote_copy(
            src_ref=coarse.at[members, rows_of, columns],
            dst_ref=maps.at[step, members, :, columns],
            send_sem=send_sem,
            recv_sem=received,
            device_id={"seg": other, "freq": band},
            device_id_type=MESH,
        ).start()

    def send_edge(step):
        send(step, edge_at, early, 0, local_segs, edge_recv.at[step // size])

    def send_rest(step):
        if width:
            send(step, rest_at, width, 0, local_segs, pair_recv.at[step // PAIR])

    def part_sem(pair, place):
        return part_recv.at[place - 1] if place else pair_recv.at[pair]

    def send_lead(group):
        pair = group * size // PAIR
        if width:
            for target, kept in enumerate(TAILS):
                send(step_to(pair, target), rest_at, width, 0, local_segs - kept, pair_recv.at[pair])

    def send_lead_passing(mine):
        pair = 3 * size // PAIR
        step = pair * PAIR
        send(step, rest_at, width - passed_columns, 0, 1, pair_recv.at[pair])
        send(step, rest_at, width, 1, local_segs - TAILS[mine] - 1, pair_recv.at[pair])
        send(step + 1, rest_at, width, 0, local_segs - TAILS[1 - mine], pair_recv.at[pair])

    def step_to(pair, target):
        return pair * PAIR + lax.rem(core + target, PAIR)

    def send_ends(group):
        pair = (group + 1) * size // PAIR - 1

        def part(place, target):
            send(step_to(pair, target), rest_at, width, begins[place], parts[place], part_sem(pair, place))

        def tail(left, target):
            step = step_to(group * size // PAIR, target)
            send(step, rest_at, width, local_segs - left, 1, tail_recv.at[left - 1])

        if width:
            for act, *args in ORDER:
                (part if act == "part" else tail)(*args)

    passes = nfreq == 2
    passed_columns = passed.shape[2]
    passed_at = bins - passed_columns

    def pass_on(source, target, ref, sent, received):
        other = partner(me, 3 * size, nseg)
        return pltpu.make_async_remote_copy(
            src_ref=source,
            dst_ref=ref,
            send_sem=sent,
            recv_sem=received,
            device_id={"seg": me if target == 0 else other, "freq": target},
            device_id_type=MESH,
        )

    def pass_first():
        rows_of = pl.ds(pl.multiple_of(partner(me, 3 * size, nseg) * rows, rows), rows)
        source = coarse.at[pl.ds(0, 1), rows_of, pl.ds(passed_at, passed_columns)]
        return pass_on(source, 0, passed, send_sem, pass_recv)

    def pass_second():
        there = maps.at[3 * size, pl.ds(0, 1), :, pl.ds(passed_at, passed_columns)]
        return pass_on(passed, 1, there, pass_send, pair_recv.at[3 * size // PAIR])

    def wait_for(there, sem):
        pltpu.make_async_copy(there, there, sem).wait()

    def wait_edges(group, first):
        wait_for(maps.at[pl.ds(group * size + first, size - first), :, :, pl.ds(0, early)], edge_recv.at[group])

    def wait_rest(step, steps, segs, sem):
        if width:
            wait_for(maps.at[pl.ds(step, steps), pl.ds(0, segs), :, pl.ds(0, width)], sem)

    def upward(group):
        members = pl.ds(group * size, size)
        return pltpu.make_async_remote_copy(
            src_ref=maps.at[members, :, :, pl.ds(bins - EDGE, EDGE)],
            dst_ref=low.at[members],
            send_sem=halo_send.at[0],
            recv_sem=halo_recv.at[0, group],
            device_id={"seg": me, "freq": band + 1},
            device_id_type=MESH,
        )

    def downward(group):
        members = pl.ds(group * size, size)
        way = halo_send.shape[0] - 1
        return pltpu.make_async_remote_copy(
            src_ref=maps.at[members, :, :, pl.ds(0, EDGE)],
            dst_ref=high.at[members],
            send_sem=halo_send.at[way],
            recv_sem=halo_recv.at[way, group],
            device_id={"seg": me, "freq": band - 1},
            device_id_type=MESH,
        )

    def forward(group):
        @pl.when(band < nfreq - 1)
        def _():
            upward(group).start()

        @pl.when(band > 0)
        def _():
            downward(group).start()

    def wait_halo(group):
        @pl.when(band < nfreq - 1)
        def _():
            downward(group).wait_recv()

        @pl.when(band > 0)
        def _():
            upward(group).wait_recv()

    barrier = pltpu.get_barrier_semaphore()

    @pl.when(inner)
    def _():
        for step in range(3 * size, 3 * size + PAIR):
            greet(step, barrier)
        for step in range(size, 2 * size):
            greet(step, barrier)
        pl.semaphore_wait(barrier, PAIR)
        for step in range(3 * size, 3 * size + PAIR):
            send_edge(step)
        if passes:
            for mine in range(PAIR):

                @pl.when(jnp.logical_and(band == 1, core == mine))
                def _():
                    send_lead_passing(mine)

            @pl.when(band == 0)
            def _():
                send_lead(3)

        else:
            send_lead(3)

    @pl.when(outer)
    def _():
        greet_bands(barrier)
        pl.semaphore_wait(barrier, size + nfreq - 1)
        each(size, 2 * size, lambda step: greet(step, near_sem))
        greet_bands(band_sem)
        each(size, 2 * size, send_edge)
        each(size, size + PAIR, send_rest)

    own = pltpu.make_async_copy(
        coarse.at[:, pl.ds(pl.multiple_of(me * rows, rows), rows), :], maps.at[0], own_sem
    )
    own.start()
    load_shifts = pltpu.make_async_copy(offsets, shifts, shifts_sem)
    load_shifts.start()
    total[...] = jnp.zeros_like(total)

    @pl.when(band == 0)
    def _():
        low[...] = jnp.zeros_like(low)

    @pl.when(band == nfreq - 1)
    def _():
        high[...] = jnp.zeros_like(high)

    @pl.when(inner)
    def _():
        pl.semaphore_wait(near_sem, size)
        greet(3 * size, far_sem)
        pl.semaphore_wait(far_sem, 1)
        greet(size, near_sem)
        each(3 * size + PAIR, nseg, send_edge)
        each(2 * size, 3 * size, send_edge)
        each(size, 2 * size, send_edge)
        each(1, size, send_edge)
        each(1, 2 * size, send_rest)
        send_lead(2)
        if nfreq > 1:
            pl.semaphore_wait(band_sem, 1)
        if passes:

            @pl.when(band == 1)
            def _():
                pass_first().start()

            @pl.when(band == 0)
            def _():
                pass_first().wait_recv()
                pass_second().start()

        each(2 * size + PAIR, 3 * size - PAIR, send_rest)
        send_ends(2)
        each(3 * size + PAIR, 4 * size - PAIR, send_rest)
        send_ends(3)

    @pl.when(outer)
    def _():
        if nfreq > 1:
            pl.semaphore_wait(band_sem, nfreq - 1)
            greet(size, band_sem)
        pl.semaphore_wait(near_sem, 1)
        each(2 * size, nseg, send_edge)
        each(1, size, send_edge)
        each(1, size, send_rest)
        each(size + PAIR, nseg, send_rest)

    lane = lax.broadcasted_iota(jnp.int32, (rows, EDGE), 1)

    def column_of(step, seg):
        return partner(me, step, nseg) * local_segs + seg

    def ring_of(step, seg):
        return jnp.where(lane < EDGE // 2, high[step, seg], low[step, seg])

    def add(lines):
        columns = [column_of(step, seg) for step, seg in lines]
        for slot, (step, seg) in enumerate(lines):
            line = jnp.concatenate([maps[step, seg], ring_of(step, seg)], axis=1)
            for shift in range(-HALO, HALO + 1):
                turned_line = line if shift == 0 else pltpu.roll(line, (-shift) % (bins + EDGE), 1)
                shifted[slot, HALO + shift] = turned_line[:, :bins]

        @pl.loop(0, spins, unroll=4)
        def _(spin):
            value = total[spin]
            for slot, column in enumerate(columns):
                value = value + shifted[slot, HALO + shifts[spin, column]]
            total[spin] = value

    tiles = bins // EDGE
    first_half = lane < CHUNK

    def turn_totals():
        @pl.loop(0, spins // 2, unroll=8)
        def _(pair):
            blocks = []
            for at in range(0, bins, EDGE):
                one = total[2 * pair, :, at : at + EDGE]
                two = total[2 * pair + 1, :, at : at + EDGE]
                blocks.append(jnp.where(first_half, one, pltpu.roll(two, CHUNK, 1)))
                blocks.append(jnp.where(first_half, pltpu.roll(one, CHUNK, 1), two))
            square = jnp.concatenate(blocks, axis=0).T
            turned[2 * pair] = square[:CHUNK]
            turned[2 * pair + 1] = square[CHUNK:]

    def turn_back():
        @pl.loop(0, spins // 2, unroll=8)
        def _(pair):
            square = jnp.concatenate([turned[2 * pair], turned[2 * pair + 1]], axis=0).T
            for tile in range(tiles):
                at = tile * EDGE
                even = square[2 * tile * rows : (2 * tile + 1) * rows]
                odd = square[(2 * tile + 1) * rows : (2 * tile + 2) * rows]
                total[2 * pair, :, at : at + EDGE] = jnp.where(first_half, even, pltpu.roll(odd, CHUNK, 1))
                total[2 * pair + 1, :, at : at + EDGE] = jnp.where(first_half, pltpu.roll(even, CHUNK, 1), odd)

    def add_turned(lines, best=None):
        columns = [column_of(step, seg) for step, seg in lines]
        own_half = lane < CHUNK + CHUNK // 2
        next_part = jnp.logical_and(lane >= CHUNK, own_half)
        for slot, (step, seg) in enumerate(lines):
            whole = [maps[step, seg, :, at : at + EDGE] for at in range(0, bins, EDGE)] + [ring_of(step, seg)]
            half = [pltpu.roll(tile, CHUNK, 1) for tile in whole]
            blocks = []
            for tile in range(tiles):
                blocks.append(jnp.where(own_half, whole[tile], whole[tile - 1]))
                blocks.append(jnp.where(next_part, half[tile + 1], half[tile]))
            square = jnp.concatenate(blocks, axis=0).T
            chunks[slot, :HALO] = square[EDGE - HALO :]
            chunks[slot, HALO:] = square[: CHUNK + HALO]

        def spindown(spin, best):
            value = turned[spin]
            for slot, column in enumerate(columns):
                value = value + chunks[slot, pl.ds(HALO + shifts[spin, column], CHUNK)]
            if best is not None:
                value = value * scale
                best = jnp.maximum(best, value)
            turned[spin] = value
            return best

        return lax.fori_loop(0, spins, spindown, best, unroll=8)

    wait_edges(1, 0)
    forward(1)
    own.wait()
    wait_edges(0, 1)
    forward(0)
    wait_edges(3, 0)
    forward(3)
    wait_edges(2, 0)
    forward(2)
    load_shifts.wait()

    pairs = size // PAIR
    opens = 3 * pairs - 1
    wait_halo(0)
    wait_rest(1, PAIR - 1, local_segs, pair_recv.at[0])

    @pl.loop(0, 4 * pairs - 1)
    def _(turn):
        group = jnp.where(turn < 2 * pairs, turn // pairs, jnp.where(turn < opens, last_group, 5 - last_group))
        member = jnp.where(turn < opens, lax.rem(turn, pairs), turn - opens)
        pair = group * pairs + member

        @pl.when(jnp.logical_and(turn > 0, member == 0))
        def _():
            wait_halo(group)

        def take(segs, waits):
            @pl.when(waits)
            def _():
                wait_rest(PAIR, PAIR, segs, pair_recv.at[pair])

            @pl.loop(0, PAIR)
            def _(core):
                add([(pair * PAIR + core, seg) for seg in range(segs)])

        @pl.when(turn != 2 * pairs)
        def _():
            take(local_segs, turn > 0)

        for target, kept in enumerate(TAILS):

            @pl.when(jnp.logical_and(turn == 2 * pairs, core == target))
            def _():
                take(local_segs - kept, True)

    def lines_of(place):
        return [(last + source, begins[place] + seg) for source in range(PAIR) for seg in range(parts[place])]

    turn_totals()
    def tails(left):
        wait_rest(PAIR, PAIR, 1, tail_recv.at[left - 1])
        return [(last_group * size + source, local_segs - left) for source in range(PAIR)]

    for place, segs in enumerate(parts):
        wait_rest(PAIR, PAIR, segs, part_sem(last // PAIR, place))
        add_turned(lines_of(place))

    @pl.when(core == PAIR - 1)
    def _():
        for left in range(TAILS[-1], 1, -1):
            add_turned(tails(left))

    best = add_turned(tails(1), jnp.full((CHUNK, EDGE), -jnp.inf, jnp.float32))
    top = best[:rows]
    for begin in range(rows, CHUNK, rows):
        top = jnp.maximum(top, best[begin : begin + rows])
    tops[0] = top

    def tell(step):
        return pltpu.make_async_remote_copy(
            src_ref=tops.at[0],
            dst_ref=tops.at[step],
            send_sem=top_send.at[step - 1],
            recv_sem=top_recv.at[step - 1],
            device_id={"seg": me, "freq": lax.rem(band + step, nfreq)},
            device_id_type=MESH,
        )

    for step in range(1, nfreq):
        tell(step).start()

    turn_back()
    sent = coarse.at[:, pl.ds(0, (nseg - 1) * rows), :]
    wait_for(sent, send_sem)

    @pl.when(band < nfreq - 1)
    def _():
        wait_for(low, halo_send.at[0])

    @pl.when(band > 0)
    def _():
        wait_for(high, halo_send.at[halo_send.shape[0] - 1])

    if passes:

        @pl.when(jnp.logical_and(inner, band == 0))
        def _():
            pass_second().wait_send()

    for step in range(1, nfreq):
        tell(step).wait()
    top = tops[0]
    for step in range(1, nfreq):
        top = jnp.maximum(top, tops[step])
    total[spins, :, :EDGE] = top


def finish(total, fine, peaks, line, sem, line_sem):
    spins, rows = fine.shape[:2]
    write = pltpu.make_async_copy(total.at[pl.ds(0, spins)], fine, sem)
    write.start()
    top = jnp.max(total[spins, :, :EDGE], axis=0, keepdims=True)
    apart = EDGE // 2
    while apart >= rows:
        top = jnp.maximum(top, pltpu.roll(top, apart, 1))
        apart //= 2
    line[...] = top[0, :rows]
    write_line = pltpu.make_async_copy(line, peaks, line_sem)
    write_line.start()
    write.wait()
    write_line.wait()


def solution(mesh):
    nseg, nfreq = mesh.shape["seg"], mesh.shape["freq"]

    def on_device(coarse, offsets):
        local_segs, points, bins = coarse.shape
        rows = points // nseg
        spins = offsets.shape[1]
        parts = (local_segs - 2, 1, 1)
        ways = 1 if nfreq <= 2 else 2
        if rows * bins != EDGE * CHUNK or nseg % (2 * PAIR * PLANES) or spins % 2:
            raise ValueError("unsupported shape")
        hbm = pl.BlockSpec(memory_space=pltpu.HBM)
        vmem = pl.BlockSpec(memory_space=pltpu.VMEM)
        dma = pltpu.SemaphoreType.DMA
        signal = pltpu.SemaphoreType.REGULAR
        total = pl.pallas_call(
            functools.partial(kernel, nseg, nfreq, parts),
            out_shape=jax.ShapeDtypeStruct((spins + 1, rows, bins), jnp.float32),
            in_specs=[hbm, hbm],
            out_specs=vmem,
            scratch_shapes=[
                pltpu.VMEM((nseg, local_segs, rows, bins), jnp.float32),
                pltpu.VMEM((nseg, local_segs, rows, EDGE), jnp.float32),
                pltpu.VMEM((nseg, local_segs, rows, EDGE), jnp.float32),
                pltpu.VMEM((local_segs, SHIFTS, rows, bins), jnp.float32),
                pltpu.VMEM((spins, CHUNK, EDGE), jnp.float32),
                pltpu.VMEM((PAIR * max(parts), CHUNK + 2 * HALO, EDGE), jnp.float32),
                pltpu.VMEM((1, rows, bins * PASSED // 8), jnp.float32),
                pltpu.VMEM((nfreq, rows, EDGE), jnp.float32),
                pltpu.SMEM(offsets.shape[::-1], jnp.int32),
                dma,
                dma,
                dma,
                dma((PLANES,)),
                dma((nseg // PAIR,)),
                dma((len(parts) - 1,)),
                dma((max(TAILS),)),
                dma((ways,)),
                dma((ways, PLANES)),
                dma((max(nfreq - 1, 1),)),
                dma((max(nfreq - 1, 1),)),
                signal,
                signal,
                signal,
                dma,
                dma,
            ],
            compiler_params=pltpu.CompilerParams(
                collective_id=0, has_side_effects=True, vmem_limit_bytes=32 << 20
            ),
        )(pltpu.with_memory_space_constraint(coarse, pltpu.HBM), pltpu.with_memory_space_constraint(offsets.T, pltpu.HBM))
        return pl.pallas_call(
            finish,
            out_shape=(
                jax.ShapeDtypeStruct((spins, rows, bins), jnp.float32),
                jax.ShapeDtypeStruct((rows,), jnp.float32),
            ),
            in_specs=[vmem],
            out_specs=(hbm, hbm),
            scratch_shapes=[pltpu.VMEM((rows,), jnp.float32), dma, dma],
            compiler_params=pltpu.CompilerParams(vmem_limit_bytes=8 << 20),
        )(total)

    return jax.shard_map(
        on_device,
        mesh=mesh,
        in_specs=(P("seg", None, "freq"), P()),
        out_specs=(P(None, "seg", "freq"), P("seg")),
        check_vma=False,
    )
```

```python
import functools

import jax
import jax.numpy as jnp
from jax import lax
from jax.experimental import pallas as pl
from jax.experimental.pallas import tpu as pltpu
from jax.sharding import PartitionSpec as P

HALO = 8
EDGE = 128
SHIFTS = 2 * HALO + 1
PLANES = 4
PAIR = 2
ORDER = (
    ("part", 0, 0),
    ("part", 0, 1),
    ("part", 1, 0),
    ("part", 2, 0),
    ("part", 1, 1),
    ("part", 2, 1),
    ("tail", 1, 0),
    ("tail", 2, 1),
    ("tail", 1, 1),
)
TAILS = (1, 2)
PASSED = 5
CHUNK = EDGE // 2
MESH = pl.DeviceIdType.MESH


def partner(me, step, count):
    result = me
    bit = 1
    while bit < count:
        wanted = (step // bit) % 2 if isinstance(step, int) else lax.rem(step // bit, 2)
        held = lax.rem(me // bit, 2)
        result = result + bit * wanted * (1 - 2 * held)
        bit *= 2
    return result


def kernel(
    nseg,
    nfreq,
    parts,
    coarse,
    offsets,
    total,
    maps,
    low,
    high,
    shifted,
    turned,
    chunks,
    passed,
    tops,
    shifts,
    own_sem,
    shifts_sem,
    send_sem,
    edge_recv,
    pair_recv,
    part_recv,
    tail_recv,
    halo_send,
    halo_recv,
    top_send,
    top_recv,
    near_sem,
    far_sem,
    band_sem,
    pass_send,
    pass_recv,
):
    local_segs = coarse.shape[0]
    spins = total.shape[0] - 1
    rows, bins = total.shape[1:]
    scale = 1.0 / (nseg * local_segs)
    size = nseg // PLANES
    begins = [sum(parts[:place]) for place in range(len(parts))]
    me = lax.axis_index("seg")
    core = lax.rem(me, PAIR)
    band = lax.axis_index("freq")
    plane = me // size
    inner = lax.rem((plane + 1) // 2, 2) == 1
    outer = jnp.logical_not(inner)
    last_group = jnp.where(inner, 3, 2)
    last = (last_group + 1) * size - PAIR

    early = EDGE if nfreq <= 2 else bins
    width = bins - early
    edge_at = jnp.where(band == 0, bins - early, 0)
    rest_at = jnp.where(band == 0, 0, early)

    def each(begin, end, act):
        @pl.loop(begin, end)
        def _(step):
            act(step)

    def greet(step, sem):
        pl.semaphore_signal(
            sem, inc=1, device_id={"seg": partner(me, step, nseg), "freq": band}, device_id_type=MESH
        )

    def greet_bands(sem):
        for step in range(1, nfreq):
            pl.semaphore_signal(
                sem, inc=1, device_id={"seg": me, "freq": lax.rem(band + step, nfreq)}, device_id_type=MESH
            )

    def send(step, begin, count, first, segs, received):
        other = partner(me, step, nseg)
        columns = pl.ds(pl.multiple_of(begin, EDGE), count)
        rows_of = pl.ds(pl.multiple_of(other * rows, rows), rows)
        members = pl.ds(first, segs)
        pltpu.make_async_remote_copy(
            src_ref=coarse.at[members, rows_of, columns],
            dst_ref=maps.at[step, members, :, columns],
            send_sem=send_sem,
            recv_sem=received,
            device_id={"seg": other, "freq": band},
            device_id_type=MESH,
        ).start()

    def send_edge(step):
        send(step, edge_at, early, 0, local_segs, edge_recv.at[step // size])

    def send_rest(step):
        if width:
            send(step, rest_at, width, 0, local_segs, pair_recv.at[step // PAIR])

    def part_sem(pair, place):
        return part_recv.at[place - 1] if place else pair_recv.at[pair]

    def send_lead(group):
        pair = group * size // PAIR
        if width:
            for target, kept in enumerate(TAILS):
                send(step_to(pair, target), rest_at, width, 0, local_segs - kept, pair_recv.at[pair])

    def send_lead_passing(mine):
        pair = 3 * size // PAIR
        step = pair * PAIR
        send(step, rest_at, width - passed_columns, 0, 1, pair_recv.at[pair])
        send(step, rest_at, width, 1, local_segs - TAILS[mine] - 1, pair_recv.at[pair])
        send(step + 1, rest_at, width, 0, local_segs - TAILS[1 - mine], pair_recv.at[pair])

    def step_to(pair, target):
        return pair * PAIR + lax.rem(core + target, PAIR)

    def send_ends(group):
        pair = (group + 1) * size // PAIR - 1

        def part(place, target):
            send(step_to(pair, target), rest_at, width, begins[place], parts[place], part_sem(pair, place))

        def tail(left, target):
            step = step_to(group * size // PAIR, target)
            send(step, rest_at, width, local_segs - left, 1, tail_recv.at[left - 1])

        if width:
            for act, *args in ORDER:
                (part if act == "part" else tail)(*args)

    passes = nfreq == 2
    passed_columns = passed.shape[2]
    passed_at = bins - passed_columns

    def pass_on(source, target, ref, sent, received):
        other = partner(me, 3 * size, nseg)
        return pltpu.make_async_remote_copy(
            src_ref=source,
            dst_ref=ref,
            send_sem=sent,
            recv_sem=received,
            device_id={"seg": me if target == 0 else other, "freq": target},
            device_id_type=MESH,
        )

    def pass_first():
        rows_of = pl.ds(pl.multiple_of(partner(me, 3 * size, nseg) * rows, rows), rows)
        source = coarse.at[pl.ds(0, 1), rows_of, pl.ds(passed_at, passed_columns)]
        return pass_on(source, 0, passed, send_sem, pass_recv)

    def pass_second():
        there = maps.at[3 * size, pl.ds(0, 1), :, pl.ds(passed_at, passed_columns)]
        return pass_on(passed, 1, there, pass_send, pair_recv.at[3 * size // PAIR])

    def wait_for(there, sem):
        pltpu.make_async_copy(there, there, sem).wait()

    def wait_edges(group, first):
        wait_for(maps.at[pl.ds(group * size + first, size - first), :, :, pl.ds(0, early)], edge_recv.at[group])

    def wait_rest(step, steps, segs, sem):
        if width:
            wait_for(maps.at[pl.ds(step, steps), pl.ds(0, segs), :, pl.ds(0, width)], sem)

    def upward(group):
        members = pl.ds(group * size, size)
        return pltpu.make_async_remote_copy(
            src_ref=maps.at[members, :, :, pl.ds(bins - EDGE, EDGE)],
            dst_ref=low.at[members],
            send_sem=halo_send.at[0],
            recv_sem=halo_recv.at[0, group],
            device_id={"seg": me, "freq": band + 1},
            device_id_type=MESH,
        )

    def downward(group):
        members = pl.ds(group * size, size)
        way = halo_send.shape[0] - 1
        return pltpu.make_async_remote_copy(
            src_ref=maps.at[members, :, :, pl.ds(0, EDGE)],
            dst_ref=high.at[members],
            send_sem=halo_send.at[way],
            recv_sem=halo_recv.at[way, group],
            device_id={"seg": me, "freq": band - 1},
            device_id_type=MESH,
        )

    def forward(group):
        @pl.when(band < nfreq - 1)
        def _():
            upward(group).start()

        @pl.when(band > 0)
        def _():
            downward(group).start()

    def wait_halo(group):
        @pl.when(band < nfreq - 1)
        def _():
            downward(group).wait_recv()

        @pl.when(band > 0)
        def _():
            upward(group).wait_recv()

    barrier = pltpu.get_barrier_semaphore()

    @pl.when(inner)
    def _():
        for step in range(3 * size, 3 * size + PAIR):
            greet(step, barrier)
        for step in range(size, 2 * size):
            greet(step, barrier)
        pl.semaphore_wait(barrier, PAIR)
        for step in range(3 * size, 3 * size + PAIR):
            send_edge(step)
        if passes:
            for mine in range(PAIR):

                @pl.when(jnp.logical_and(band == 1, core == mine))
                def _():
                    send_lead_passing(mine)

            @pl.when(band == 0)
            def _():
                send_lead(3)

        else:
            send_lead(3)

    @pl.when(outer)
    def _():
        greet_bands(barrier)
        pl.semaphore_wait(barrier, size + nfreq - 1)
        each(size, 2 * size, lambda step: greet(step, near_sem))
        greet_bands(band_sem)
        each(size, 2 * size, send_edge)
        each(size, size + PAIR, send_rest)

    own = pltpu.make_async_copy(
        coarse.at[:, pl.ds(pl.multiple_of(me * rows, rows), rows), :], maps.at[0], own_sem
    )
    own.start()
    load_shifts = pltpu.make_async_copy(offsets, shifts, shifts_sem)
    load_shifts.start()
    total[...] = jnp.zeros_like(total)

    @pl.when(band == 0)
    def _():
        low[...] = jnp.zeros_like(low)

    @pl.when(band == nfreq - 1)
    def _():
        high[...] = jnp.zeros_like(high)

    @pl.when(inner)
    def _():
        pl.semaphore_wait(near_sem, size)
        greet(3 * size, far_sem)
        pl.semaphore_wait(far_sem, 1)
        greet(size, near_sem)
        each(3 * size + PAIR, nseg, send_edge)
        each(2 * size, 3 * size, send_edge)
        each(size, 2 * size, send_edge)
        each(1, size, send_edge)
        each(1, 2 * size, send_rest)
        send_lead(2)
        if nfreq > 1:
            pl.semaphore_wait(band_sem, 1)
        if passes:

            @pl.when(band == 1)
            def _():
                pass_first().start()

            @pl.when(band == 0)
            def _():
                pass_first().wait_recv()
                pass_second().start()

        each(2 * size + PAIR, 3 * size - PAIR, send_rest)
        send_ends(2)
        each(3 * size + PAIR, 4 * size - PAIR, send_rest)
        send_ends(3)

    @pl.when(outer)
    def _():
        if nfreq > 1:
            pl.semaphore_wait(band_sem, nfreq - 1)
            greet(size, band_sem)
        pl.semaphore_wait(near_sem, 1)
        each(2 * size, nseg, send_edge)
        each(1, size, send_edge)
        each(1, size, send_rest)
        each(size + PAIR, nseg, send_rest)

    lane = lax.broadcasted_iota(jnp.int32, (rows, EDGE), 1)

    def column_of(step, seg):
        return partner(me, step, nseg) * local_segs + seg

    def ring_of(step, seg):
        return jnp.where(lane < EDGE // 2, high[step, seg], low[step, seg])

    def add(lines):
        columns = [column_of(step, seg) for step, seg in lines]
        for slot, (step, seg) in enumerate(lines):
            line = jnp.concatenate([maps[step, seg], ring_of(step, seg)], axis=1)
            for shift in range(-HALO, HALO + 1):
                turned_line = line if shift == 0 else pltpu.roll(line, (-shift) % (bins + EDGE), 1)
                shifted[slot, HALO + shift] = turned_line[:, :bins]

        @pl.loop(0, spins, unroll=4)
        def _(spin):
            value = total[spin]
            for slot, column in enumerate(columns):
                value = value + shifted[slot, HALO + shifts[spin, column]]
            total[spin] = value

    tiles = bins // EDGE
    first_half = lane < CHUNK

    def turn_totals():
        @pl.loop(0, spins // 2, unroll=8)
        def _(pair):
            blocks = []
            for at in range(0, bins, EDGE):
                one = total[2 * pair, :, at : at + EDGE]
                two = total[2 * pair + 1, :, at : at + EDGE]
                blocks.append(jnp.where(first_half, one, pltpu.roll(two, CHUNK, 1)))
                blocks.append(jnp.where(first_half, pltpu.roll(one, CHUNK, 1), two))
            square = jnp.concatenate(blocks, axis=0).T
            turned[2 * pair] = square[:CHUNK]
            turned[2 * pair + 1] = square[CHUNK:]

    def turn_back():
        @pl.loop(0, spins // 2, unroll=8)
        def _(pair):
            square = jnp.concatenate([turned[2 * pair], turned[2 * pair + 1]], axis=0).T
            for tile in range(tiles):
                at = tile * EDGE
                even = square[2 * tile * rows : (2 * tile + 1) * rows]
                odd = square[(2 * tile + 1) * rows : (2 * tile + 2) * rows]
                total[2 * pair, :, at : at + EDGE] = jnp.where(first_half, even, pltpu.roll(odd, CHUNK, 1))
                total[2 * pair + 1, :, at : at + EDGE] = jnp.where(first_half, pltpu.roll(even, CHUNK, 1), odd)

    def add_turned(lines, best=None):
        columns = [column_of(step, seg) for step, seg in lines]
        own_half = lane < CHUNK + CHUNK // 2
        next_part = jnp.logical_and(lane >= CHUNK, own_half)
        for slot, (step, seg) in enumerate(lines):
            whole = [maps[step, seg, :, at : at + EDGE] for at in range(0, bins, EDGE)] + [ring_of(step, seg)]
            half = [pltpu.roll(tile, CHUNK, 1) for tile in whole]
            blocks = []
            for tile in range(tiles):
                blocks.append(jnp.where(own_half, whole[tile], whole[tile - 1]))
                blocks.append(jnp.where(next_part, half[tile + 1], half[tile]))
            square = jnp.concatenate(blocks, axis=0).T
            chunks[slot, :HALO] = square[EDGE - HALO :]
            chunks[slot, HALO:] = square[: CHUNK + HALO]

        def spindown(spin, best):
            value = turned[spin]
            for slot, column in enumerate(columns):
                value = value + chunks[slot, pl.ds(HALO + shifts[spin, column], CHUNK)]
            if best is not None:
                value = value * scale
                best = jnp.maximum(best, value)
            turned[spin] = value
            return best

        return lax.fori_loop(0, spins, spindown, best, unroll=8)

    wait_edges(1, 0)
    forward(1)
    own.wait()
    wait_edges(0, 1)
    forward(0)
    wait_edges(3, 0)
    forward(3)
    wait_edges(2, 0)
    forward(2)
    load_shifts.wait()

    pairs = size // PAIR
    opens = 3 * pairs - 1
    wait_halo(0)
    wait_rest(1, PAIR - 1, local_segs, pair_recv.at[0])

    @pl.loop(0, 4 * pairs - 1)
    def _(turn):
        group = jnp.where(turn < 2 * pairs, turn // pairs, jnp.where(turn < opens, last_group, 5 - last_group))
        member = jnp.where(turn < opens, lax.rem(turn, pairs), turn - opens)
        pair = group * pairs + member

        @pl.when(jnp.logical_and(turn > 0, member == 0))
        def _():
            wait_halo(group)

        def take(segs, waits):
            @pl.when(waits)
            def _():
                wait_rest(PAIR, PAIR, segs, pair_recv.at[pair])

            @pl.loop(0, PAIR)
            def _(core):
                add([(pair * PAIR + core, seg) for seg in range(segs)])

        @pl.when(turn != 2 * pairs)
        def _():
            take(local_segs, turn > 0)

        for target, kept in enumerate(TAILS):

            @pl.when(jnp.logical_and(turn == 2 * pairs, core == target))
            def _():
                take(local_segs - kept, True)

    def lines_of(place):
        return [(last + source, begins[place] + seg) for source in range(PAIR) for seg in range(parts[place])]

    turn_totals()
    def tails(left):
        wait_rest(PAIR, PAIR, 1, tail_recv.at[left - 1])
        return [(last_group * size + source, local_segs - left) for source in range(PAIR)]

    for place, segs in enumerate(parts):
        wait_rest(PAIR, PAIR, segs, part_sem(last // PAIR, place))
        if place < len(parts) - 1:
            add_turned(lines_of(place))

    for target, kept in enumerate(TAILS):

        @pl.when(core == target)
        def _():
            lines = lines_of(len(parts) - 1)
            for left in range(kept, 1, -1):
                lines = lines + tails(left)
            add_turned(lines)

    best = add_turned(tails(1), jnp.full((CHUNK, EDGE), -jnp.inf, jnp.float32))
    top = best[:rows]
    for begin in range(rows, CHUNK, rows):
        top = jnp.maximum(top, best[begin : begin + rows])
    tops[0] = top

    def tell(step):
        return pltpu.make_async_remote_copy(
            src_ref=tops.at[0],
            dst_ref=tops.at[step],
            send_sem=top_send.at[step - 1],
            recv_sem=top_recv.at[step - 1],
            device_id={"seg": me, "freq": lax.rem(band + step, nfreq)},
            device_id_type=MESH,
        )

    for step in range(1, nfreq):
        tell(step).start()

    turn_back()
    sent = coarse.at[:, pl.ds(0, (nseg - 1) * rows), :]
    wait_for(sent, send_sem)

    @pl.when(band < nfreq - 1)
    def _():
        wait_for(low, halo_send.at[0])

    @pl.when(band > 0)
    def _():
        wait_for(high, halo_send.at[halo_send.shape[0] - 1])

    if passes:

        @pl.when(jnp.logical_and(inner, band == 0))
        def _():
            pass_second().wait_send()

    for step in range(1, nfreq):
        tell(step).wait()
    top = tops[0]
    for step in range(1, nfreq):
        top = jnp.maximum(top, tops[step])
    total[spins, :, :EDGE] = top


def finish(total, fine, peaks, line, sem, line_sem):
    spins, rows = fine.shape[:2]
    write = pltpu.make_async_copy(total.at[pl.ds(0, spins)], fine, sem)
    write.start()
    top = jnp.max(total[spins, :, :EDGE], axis=0, keepdims=True)
    apart = EDGE // 2
    while apart >= rows:
        top = jnp.maximum(top, pltpu.roll(top, apart, 1))
        apart //= 2
    line[...] = top[0, :rows]
    write_line = pltpu.make_async_copy(line, peaks, line_sem)
    write_line.start()
    write.wait()
    write_line.wait()


def solution(mesh):
    nseg, nfreq = mesh.shape["seg"], mesh.shape["freq"]

    def on_device(coarse, offsets):
        local_segs, points, bins = coarse.shape
        rows = points // nseg
        spins = offsets.shape[1]
        parts = (local_segs - 2, 1, 1)
        ways = 1 if nfreq <= 2 else 2
        if rows * bins != EDGE * CHUNK or nseg % (2 * PAIR * PLANES) or spins % 2:
            raise ValueError("unsupported shape")
        hbm = pl.BlockSpec(memory_space=pltpu.HBM)
        vmem = pl.BlockSpec(memory_space=pltpu.VMEM)
        dma = pltpu.SemaphoreType.DMA
        signal = pltpu.SemaphoreType.REGULAR
        total = pl.pallas_call(
            functools.partial(kernel, nseg, nfreq, parts),
            out_shape=jax.ShapeDtypeStruct((spins + 1, rows, bins), jnp.float32),
            in_specs=[hbm, hbm],
            out_specs=vmem,
            scratch_shapes=[
                pltpu.VMEM((nseg, local_segs, rows, bins), jnp.float32),
                pltpu.VMEM((nseg, local_segs, rows, EDGE), jnp.float32),
                pltpu.VMEM((nseg, local_segs, rows, EDGE), jnp.float32),
                pltpu.VMEM((local_segs, SHIFTS, rows, bins), jnp.float32),
                pltpu.VMEM((spins, CHUNK, EDGE), jnp.float32),
                pltpu.VMEM((PAIR * max(parts), CHUNK + 2 * HALO, EDGE), jnp.float32),
                pltpu.VMEM((1, rows, bins * PASSED // 8), jnp.float32),
                pltpu.VMEM((nfreq, rows, EDGE), jnp.float32),
                pltpu.SMEM(offsets.shape[::-1], jnp.int32),
                dma,
                dma,
                dma,
                dma((PLANES,)),
                dma((nseg // PAIR,)),
                dma((len(parts) - 1,)),
                dma((max(TAILS),)),
                dma((ways,)),
                dma((ways, PLANES)),
                dma((max(nfreq - 1, 1),)),
                dma((max(nfreq - 1, 1),)),
                signal,
                signal,
                signal,
                dma,
                dma,
            ],
            compiler_params=pltpu.CompilerParams(
                collective_id=0, has_side_effects=True, vmem_limit_bytes=32 << 20
            ),
        )(pltpu.with_memory_space_constraint(coarse, pltpu.HBM), pltpu.with_memory_space_constraint(offsets.T, pltpu.HBM))
        return pl.pallas_call(
            finish,
            out_shape=(
                jax.ShapeDtypeStruct((spins, rows, bins), jnp.float32),
                jax.ShapeDtypeStruct((rows,), jnp.float32),
            ),
            in_specs=[vmem],
            out_specs=(hbm, hbm),
            scratch_shapes=[pltpu.VMEM((rows,), jnp.float32), dma, dma],
            compiler_params=pltpu.CompilerParams(vmem_limit_bytes=8 << 20),
        )(total)

    return jax.shard_map(
        on_device,
        mesh=mesh,
        in_specs=(P("seg", None, "freq"), P()),
        out_specs=(P(None, "seg", "freq"), P("seg")),
        check_vma=False,
    )
```

```python
import functools

import jax
import jax.numpy as jnp
from jax import lax
from jax.experimental import pallas as pl
from jax.experimental.pallas import tpu as pltpu
from jax.sharding import PartitionSpec as P

HALO = 8
EDGE = 128
SHIFTS = 2 * HALO + 1
PLANES = 4
PAIR = 2
ORDER = (
    ("part", 0, 0),
    ("part", 0, 1),
    ("part", 1, 0),
    ("part", 2, 0),
    ("part", 1, 1),
    ("part", 2, 1),
    ("tail", 1, 0),
    ("tail", 2, 1),
    ("tail", 1, 1),
)
TAILS = (1, 2)
PASSED = 5
CHUNK = EDGE // 2
MESH = pl.DeviceIdType.MESH


def partner(me, step, count):
    result = me
    bit = 1
    while bit < count:
        wanted = (step // bit) % 2 if isinstance(step, int) else lax.rem(step // bit, 2)
        held = lax.rem(me // bit, 2)
        result = result + bit * wanted * (1 - 2 * held)
        bit *= 2
    return result


def kernel(
    nseg,
    nfreq,
    parts,
    coarse,
    offsets,
    total,
    maps,
    low,
    high,
    shifted,
    turned,
    chunks,
    passed,
    ahead,
    tops,
    shifts,
    own_sem,
    shifts_sem,
    send_sem,
    edge_recv,
    pair_recv,
    part_recv,
    tail_recv,
    halo_send,
    halo_recv,
    top_send,
    top_recv,
    near_sem,
    far_sem,
    band_sem,
    pass_send,
    pass_recv,
    ahead_sem,
):
    local_segs = coarse.shape[0]
    spins = total.shape[0] - 1
    rows, bins = total.shape[1:]
    scale = 1.0 / (nseg * local_segs)
    size = nseg // PLANES
    begins = [sum(parts[:place]) for place in range(len(parts))]
    me = lax.axis_index("seg")
    core = lax.rem(me, PAIR)
    band = lax.axis_index("freq")
    plane = me // size
    inner = lax.rem((plane + 1) // 2, 2) == 1
    outer = jnp.logical_not(inner)
    last_group = jnp.where(inner, 3, 2)
    last = (last_group + 1) * size - PAIR

    early = EDGE if nfreq <= 2 else bins
    width = bins - early
    edge_at = jnp.where(band == 0, bins - early, 0)
    rest_at = jnp.where(band == 0, 0, early)

    def each(begin, end, act):
        @pl.loop(begin, end)
        def _(step):
            act(step)

    def greet(step, sem):
        pl.semaphore_signal(
            sem, inc=1, device_id={"seg": partner(me, step, nseg), "freq": band}, device_id_type=MESH
        )

    def greet_bands(sem):
        for step in range(1, nfreq):
            pl.semaphore_signal(
                sem, inc=1, device_id={"seg": me, "freq": lax.rem(band + step, nfreq)}, device_id_type=MESH
            )

    def send(step, begin, count, first, segs, received, held=None):
        other = partner(me, step, nseg)
        columns = pl.ds(pl.multiple_of(begin, EDGE), count)
        rows_of = pl.ds(pl.multiple_of(other * rows, rows), rows)
        members = pl.ds(first, segs)
        pltpu.make_async_remote_copy(
            src_ref=coarse.at[members, rows_of, columns] if held is None else held.at[step - 3 * size, members, :, columns],
            dst_ref=maps.at[step, members, :, columns],
            send_sem=send_sem,
            recv_sem=received,
            device_id={"seg": other, "freq": band},
            device_id_type=MESH,
        ).start()

    def send_edge(step, held=None):
        send(step, edge_at, early, 0, local_segs, edge_recv.at[step // size], held)

    def send_rest(step):
        if width:
            send(step, rest_at, width, 0, local_segs, pair_recv.at[step // PAIR])

    def part_sem(pair, place):
        return part_recv.at[place - 1] if place else pair_recv.at[pair]

    def send_lead(group, held=None):
        pair = group * size // PAIR
        if width:
            for target, kept in enumerate(TAILS):
                send(step_to(pair, target), rest_at, width, 0, local_segs - kept, pair_recv.at[pair], held)

    def send_lead_passing(mine, held):
        pair = 3 * size // PAIR
        step = pair * PAIR
        send(step, rest_at, width - passed_columns, 0, 1, pair_recv.at[pair], held)
        send(step, rest_at, width, 1, local_segs - TAILS[mine] - 1, pair_recv.at[pair], held)
        send(step + 1, rest_at, width, 0, local_segs - TAILS[1 - mine], pair_recv.at[pair], held)

    def step_to(pair, target):
        return pair * PAIR + lax.rem(core + target, PAIR)

    def send_ends(group):
        pair = (group + 1) * size // PAIR - 1

        def part(place, target):
            send(step_to(pair, target), rest_at, width, begins[place], parts[place], part_sem(pair, place))

        def tail(left, target):
            step = step_to(group * size // PAIR, target)
            send(step, rest_at, width, local_segs - left, 1, tail_recv.at[left - 1])

        if width:
            for act, *args in ORDER:
                (part if act == "part" else tail)(*args)

    passes = nfreq == 2
    passed_columns = passed.shape[2]
    passed_at = bins - passed_columns

    def pass_on(source, target, ref, sent, received):
        other = partner(me, 3 * size, nseg)
        return pltpu.make_async_remote_copy(
            src_ref=source,
            dst_ref=ref,
            send_sem=sent,
            recv_sem=received,
            device_id={"seg": me if target == 0 else other, "freq": target},
            device_id_type=MESH,
        )

    def pass_first():
        rows_of = pl.ds(pl.multiple_of(partner(me, 3 * size, nseg) * rows, rows), rows)
        source = coarse.at[pl.ds(0, 1), rows_of, pl.ds(passed_at, passed_columns)]
        return pass_on(source, 0, passed, send_sem, pass_recv)

    def pass_second():
        there = maps.at[3 * size, pl.ds(0, 1), :, pl.ds(passed_at, passed_columns)]
        return pass_on(passed, 1, there, pass_send, pair_recv.at[3 * size // PAIR])

    def wait_for(there, sem):
        pltpu.make_async_copy(there, there, sem).wait()

    def wait_edges(group, first):
        wait_for(maps.at[pl.ds(group * size + first, size - first), :, :, pl.ds(0, early)], edge_recv.at[group])

    def wait_rest(step, steps, segs, sem):
        if width:
            wait_for(maps.at[pl.ds(step, steps), pl.ds(0, segs), :, pl.ds(0, width)], sem)

    def upward(group):
        members = pl.ds(group * size, size)
        return pltpu.make_async_remote_copy(
            src_ref=maps.at[members, :, :, pl.ds(bins - EDGE, EDGE)],
            dst_ref=low.at[members],
            send_sem=halo_send.at[0],
            recv_sem=halo_recv.at[0, group],
            device_id={"seg": me, "freq": band + 1},
            device_id_type=MESH,
        )

    def downward(group):
        members = pl.ds(group * size, size)
        way = halo_send.shape[0] - 1
        return pltpu.make_async_remote_copy(
            src_ref=maps.at[members, :, :, pl.ds(0, EDGE)],
            dst_ref=high.at[members],
            send_sem=halo_send.at[way],
            recv_sem=halo_recv.at[way, group],
            device_id={"seg": me, "freq": band - 1},
            device_id_type=MESH,
        )

    def forward(group):
        @pl.when(band < nfreq - 1)
        def _():
            upward(group).start()

        @pl.when(band > 0)
        def _():
            downward(group).start()

    def wait_halo(group):
        @pl.when(band < nfreq - 1)
        def _():
            downward(group).wait_recv()

        @pl.when(band > 0)
        def _():
            upward(group).wait_recv()

    def send_first(held):
        for step in range(3 * size, 3 * size + PAIR):
            send_edge(step, held)
        if passes:
            for mine in range(PAIR):

                @pl.when(jnp.logical_and(band == 1, core == mine))
                def _():
                    send_lead_passing(mine, held)

            @pl.when(band == 0)
            def _():
                send_lead(3, held)

        else:
            send_lead(3, held)

    barrier = pltpu.get_barrier_semaphore()

    @pl.when(inner)
    def _():
        for step in range(3 * size, 3 * size + PAIR):
            greet(step, barrier)
        for step in range(size, 2 * size):
            greet(step, barrier)

        @pl.when(plane == 1)
        def _():
            for step in range(PAIR):
                rows_of = pl.ds(pl.multiple_of(partner(me, 3 * size + step, nseg) * rows, rows), rows)
                pltpu.make_async_copy(coarse.at[:, rows_of, :], ahead.at[step], ahead_sem).start()

        pl.semaphore_wait(barrier, PAIR)

        @pl.when(plane == 1)
        def _():
            wait_for(ahead, ahead_sem)
            send_first(ahead)

        @pl.when(plane == 2)
        def _():
            send_first(None)

    @pl.when(outer)
    def _():
        greet_bands(barrier)
        pl.semaphore_wait(barrier, size + nfreq - 1)
        each(size, 2 * size, lambda step: greet(step, near_sem))
        greet_bands(band_sem)
        each(size, 2 * size, send_edge)
        each(size, size + PAIR, send_rest)

    own = pltpu.make_async_copy(
        coarse.at[:, pl.ds(pl.multiple_of(me * rows, rows), rows), :], maps.at[0], own_sem
    )
    own.start()
    load_shifts = pltpu.make_async_copy(offsets, shifts, shifts_sem)
    load_shifts.start()
    total[...] = jnp.zeros_like(total)

    @pl.when(band == 0)
    def _():
        low[...] = jnp.zeros_like(low)

    @pl.when(band == nfreq - 1)
    def _():
        high[...] = jnp.zeros_like(high)

    @pl.when(inner)
    def _():
        pl.semaphore_wait(near_sem, size)
        greet(3 * size, far_sem)
        pl.semaphore_wait(far_sem, 1)
        greet(size, near_sem)
        each(3 * size + PAIR, nseg, send_edge)
        each(2 * size, 3 * size, send_edge)
        each(size, 2 * size, send_edge)
        each(1, size, send_edge)
        each(1, 2 * size, send_rest)
        send_lead(2)
        if nfreq > 1:
            pl.semaphore_wait(band_sem, 1)
        if passes:

            @pl.when(band == 1)
            def _():
                pass_first().start()

            @pl.when(band == 0)
            def _():
                pass_first().wait_recv()
                pass_second().start()

        each(2 * size + PAIR, 3 * size - PAIR, send_rest)
        send_ends(2)
        each(3 * size + PAIR, 4 * size - PAIR, send_rest)
        send_ends(3)

    @pl.when(outer)
    def _():
        if nfreq > 1:
            pl.semaphore_wait(band_sem, nfreq - 1)
            greet(size, band_sem)
        pl.semaphore_wait(near_sem, 1)
        each(2 * size, nseg, send_edge)
        each(1, size, send_edge)
        each(1, size, send_rest)
        each(size + PAIR, nseg, send_rest)

    lane = lax.broadcasted_iota(jnp.int32, (rows, EDGE), 1)

    def column_of(step, seg):
        return partner(me, step, nseg) * local_segs + seg

    def ring_of(step, seg):
        return jnp.where(lane < EDGE // 2, high[step, seg], low[step, seg])

    def add(lines):
        columns = [column_of(step, seg) for step, seg in lines]
        for slot, (step, seg) in enumerate(lines):
            line = jnp.concatenate([maps[step, seg], ring_of(step, seg)], axis=1)
            for shift in range(-HALO, HALO + 1):
                turned_line = line if shift == 0 else pltpu.roll(line, (-shift) % (bins + EDGE), 1)
                shifted[slot, HALO + shift] = turned_line[:, :bins]

        @pl.loop(0, spins, unroll=4)
        def _(spin):
            value = total[spin]
            for slot, column in enumerate(columns):
                value = value + shifted[slot, HALO + shifts[spin, column]]
            total[spin] = value

    tiles = bins // EDGE
    first_half = lane < CHUNK

    def turn_totals():
        @pl.loop(0, spins // 2, unroll=8)
        def _(pair):
            blocks = []
            for at in range(0, bins, EDGE):
                one = total[2 * pair, :, at : at + EDGE]
                two = total[2 * pair + 1, :, at : at + EDGE]
                blocks.append(jnp.where(first_half, one, pltpu.roll(two, CHUNK, 1)))
                blocks.append(jnp.where(first_half, pltpu.roll(one, CHUNK, 1), two))
            square = jnp.concatenate(blocks, axis=0).T
            turned[2 * pair] = square[:CHUNK]
            turned[2 * pair + 1] = square[CHUNK:]

    def turn_back():
        @pl.loop(0, spins // 2, unroll=8)
        def _(pair):
            square = jnp.concatenate([turned[2 * pair], turned[2 * pair + 1]], axis=0).T
            for tile in range(tiles):
                at = tile * EDGE
                even = square[2 * tile * rows : (2 * tile + 1) * rows]
                odd = square[(2 * tile + 1) * rows : (2 * tile + 2) * rows]
                total[2 * pair, :, at : at + EDGE] = jnp.where(first_half, even, pltpu.roll(odd, CHUNK, 1))
                total[2 * pair + 1, :, at : at + EDGE] = jnp.where(first_half, pltpu.roll(even, CHUNK, 1), odd)

    def add_turned(lines, best=None):
        columns = [column_of(step, seg) for step, seg in lines]
        own_half = lane < CHUNK + CHUNK // 2
        next_part = jnp.logical_and(lane >= CHUNK, own_half)
        for slot, (step, seg) in enumerate(lines):
            whole = [maps[step, seg, :, at : at + EDGE] for at in range(0, bins, EDGE)] + [ring_of(step, seg)]
            half = [pltpu.roll(tile, CHUNK, 1) for tile in whole]
            blocks = []
            for tile in range(tiles):
                blocks.append(jnp.where(own_half, whole[tile], whole[tile - 1]))
                blocks.append(jnp.where(next_part, half[tile + 1], half[tile]))
            square = jnp.concatenate(blocks, axis=0).T
            chunks[slot, :HALO] = square[EDGE - HALO :]
            chunks[slot, HALO:] = square[: CHUNK + HALO]

        def spindown(spin, best):
            value = turned[spin]
            for slot, column in enumerate(columns):
                value = value + chunks[slot, pl.ds(HALO + shifts[spin, column], CHUNK)]
            if best is not None:
                value = value * scale
                best = jnp.maximum(best, value)
            turned[spin] = value
            return best

        return lax.fori_loop(0, spins, spindown, best, unroll=8)

    wait_edges(1, 0)
    forward(1)
    own.wait()
    wait_edges(0, 1)
    forward(0)
    wait_edges(3, 0)
    forward(3)
    wait_edges(2, 0)
    forward(2)
    load_shifts.wait()

    pairs = size // PAIR
    opens = 3 * pairs - 1
    wait_halo(0)
    wait_rest(1, PAIR - 1, local_segs, pair_recv.at[0])

    @pl.loop(0, 4 * pairs - 1)
    def _(turn):
        group = jnp.where(turn < 2 * pairs, turn // pairs, jnp.where(turn < opens, last_group, 5 - last_group))
        member = jnp.where(turn < opens, lax.rem(turn, pairs), turn - opens)
        pair = group * pairs + member

        @pl.when(jnp.logical_and(turn > 0, member == 0))
        def _():
            wait_halo(group)

        def take(segs, waits):
            @pl.when(waits)
            def _():
                wait_rest(PAIR, PAIR, segs, pair_recv.at[pair])

            @pl.loop(0, PAIR)
            def _(core):
                add([(pair * PAIR + core, seg) for seg in range(segs)])

        @pl.when(turn != 2 * pairs)
        def _():
            take(local_segs, turn > 0)

        for target, kept in enumerate(TAILS):

            @pl.when(jnp.logical_and(turn == 2 * pairs, core == target))
            def _():
                take(local_segs - kept, True)

    def lines_of(place):
        return [(last + source, begins[place] + seg) for source in range(PAIR) for seg in range(parts[place])]

    turn_totals()
    def tails(left):
        wait_rest(PAIR, PAIR, 1, tail_recv.at[left - 1])
        return [(last_group * size + source, local_segs - left) for source in range(PAIR)]

    for place, segs in enumerate(parts):
        wait_rest(PAIR, PAIR, segs, part_sem(last // PAIR, place))
        if place < len(parts) - 1:
            add_turned(lines_of(place))

    for target, kept in enumerate(TAILS):

        @pl.when(core == target)
        def _():
            lines = lines_of(len(parts) - 1)
            for left in range(kept, 1, -1):
                lines = lines + tails(left)
            add_turned(lines)

    best = add_turned(tails(1), jnp.full((CHUNK, EDGE), -jnp.inf, jnp.float32))
    top = best[:rows]
    for begin in range(rows, CHUNK, rows):
        top = jnp.maximum(top, best[begin : begin + rows])
    tops[0] = top

    def tell(step):
        return pltpu.make_async_remote_copy(
            src_ref=tops.at[0],
            dst_ref=tops.at[step],
            send_sem=top_send.at[step - 1],
            recv_sem=top_recv.at[step - 1],
            device_id={"seg": me, "freq": lax.rem(band + step, nfreq)},
            device_id_type=MESH,
        )

    for step in range(1, nfreq):
        tell(step).start()

    turn_back()
    sent = coarse.at[:, pl.ds(0, (nseg - 1) * rows), :]
    wait_for(sent, send_sem)

    @pl.when(band < nfreq - 1)
    def _():
        wait_for(low, halo_send.at[0])

    @pl.when(band > 0)
    def _():
        wait_for(high, halo_send.at[halo_send.shape[0] - 1])

    if passes:

        @pl.when(jnp.logical_and(inner, band == 0))
        def _():
            pass_second().wait_send()

    for step in range(1, nfreq):
        tell(step).wait()
    top = tops[0]
    for step in range(1, nfreq):
        top = jnp.maximum(top, tops[step])
    total[spins, :, :EDGE] = top


def finish(total, fine, peaks, line, sem, line_sem):
    spins, rows = fine.shape[:2]
    write = pltpu.make_async_copy(total.at[pl.ds(0, spins)], fine, sem)
    write.start()
    top = jnp.max(total[spins, :, :EDGE], axis=0, keepdims=True)
    apart = EDGE // 2
    while apart >= rows:
        top = jnp.maximum(top, pltpu.roll(top, apart, 1))
        apart //= 2
    line[...] = top[0, :rows]
    write_line = pltpu.make_async_copy(line, peaks, line_sem)
    write_line.start()
    write.wait()
    write_line.wait()


def solution(mesh):
    nseg, nfreq = mesh.shape["seg"], mesh.shape["freq"]

    def on_device(coarse, offsets):
        local_segs, points, bins = coarse.shape
        rows = points // nseg
        spins = offsets.shape[1]
        parts = (local_segs - 2, 1, 1)
        ways = 1 if nfreq <= 2 else 2
        if rows * bins != EDGE * CHUNK or nseg % (2 * PAIR * PLANES) or spins % 2:
            raise ValueError("unsupported shape")
        hbm = pl.BlockSpec(memory_space=pltpu.HBM)
        vmem = pl.BlockSpec(memory_space=pltpu.VMEM)
        dma = pltpu.SemaphoreType.DMA
        signal = pltpu.SemaphoreType.REGULAR
        total = pl.pallas_call(
            functools.partial(kernel, nseg, nfreq, parts),
            out_shape=jax.ShapeDtypeStruct((spins + 1, rows, bins), jnp.float32),
            in_specs=[hbm, hbm],
            out_specs=vmem,
            scratch_shapes=[
                pltpu.VMEM((nseg, local_segs, rows, bins), jnp.float32),
                pltpu.VMEM((nseg, local_segs, rows, EDGE), jnp.float32),
                pltpu.VMEM((nseg, local_segs, rows, EDGE), jnp.float32),
                pltpu.VMEM((local_segs, SHIFTS, rows, bins), jnp.float32),
                pltpu.VMEM((spins, CHUNK, EDGE), jnp.float32),
                pltpu.VMEM((PAIR * max(parts), CHUNK + 2 * HALO, EDGE), jnp.float32),
                pltpu.VMEM((1, rows, bins * PASSED // 8), jnp.float32),
                pltpu.VMEM((PAIR, local_segs, rows, bins), jnp.float32),
                pltpu.VMEM((nfreq, rows, EDGE), jnp.float32),
                pltpu.SMEM(offsets.shape[::-1], jnp.int32),
                dma,
                dma,
                dma,
                dma((PLANES,)),
                dma((nseg // PAIR,)),
                dma((len(parts) - 1,)),
                dma((max(TAILS),)),
                dma((ways,)),
                dma((ways, PLANES)),
                dma((max(nfreq - 1, 1),)),
                dma((max(nfreq - 1, 1),)),
                signal,
                signal,
                signal,
                dma,
                dma,
                dma,
            ],
            compiler_params=pltpu.CompilerParams(
                collective_id=0, has_side_effects=True, vmem_limit_bytes=32 << 20
            ),
        )(pltpu.with_memory_space_constraint(coarse, pltpu.HBM), pltpu.with_memory_space_constraint(offsets.T, pltpu.HBM))
        return pl.pallas_call(
            finish,
            out_shape=(
                jax.ShapeDtypeStruct((spins, rows, bins), jnp.float32),
                jax.ShapeDtypeStruct((rows,), jnp.float32),
            ),
            in_specs=[vmem],
            out_specs=(hbm, hbm),
            scratch_shapes=[pltpu.VMEM((rows,), jnp.float32), dma, dma],
            compiler_params=pltpu.CompilerParams(vmem_limit_bytes=8 << 20),
        )(total)

    return jax.shard_map(
        on_device,
        mesh=mesh,
        in_specs=(P("seg", None, "freq"), P()),
        out_specs=(P(None, "seg", "freq"), P("seg")),
        check_vma=False,
    )
```
